32 devices in a mesh: dp: 8 (over y, x, core), vocab: 4 (over z).
Axes of the slice: x: 2, y: 2, z: 4, core: 2. Of those that a mesh axis runs over, the one named last changes fastest.
Arguments:
- resid: bfloat16 [2, 1024, 4096], P(None, 'dp'), may hold values from -6 to 6
- norm_gain: float32 [4096], replicated, may hold values from 0.5 to 1.5
- in_x: bfloat16 [4096, 4096], P('dp', 'vocab'), may hold values from -0.09375 to 0.09375
- in_z: bfloat16 [4096, 4096], P('dp', 'vocab'), may hold values from -0.09375 to 0.09375
- conv_w: float32 [4, 4096], P(None, 'vocab'), may hold values from -3 to 3
- conv_b: float32 [4096], P('vocab'), may hold values from -3 to 3
- xdt_w: bfloat16 [4096, 256], P('vocab'), may hold values from -0.09375 to 0.09375
- xbc_w: bfloat16 [4096, 32], P('vocab'), may hold values from -0.09375 to 0.09375
- dt_gain: float32 [256], replicated, may hold values from 0.5 to 1.5
- dt_proj: bfloat16 [256, 4096], P(None, 'vocab'), may hold values from -0.375 to 0.375
- dt_bias: float32 [4096], P('vocab'), may hold values from -4 to 1
- a_rate: float32 [4096, 16], P('vocab'), may hold values from 0.0001 to 1
- out_w: bfloat16 [4096, 4096], P('vocab'), may hold values from -0.09375 to 0.09375
- final_gain: float32 [4096], replicated, may hold values from 0.5 to 1.5
- head_w: bfloat16 [8192, 4096], P('vocab', 'dp'), as said below
- targets: int32 [2, 1024], P(None, 'dp'), may hold values from 0 to 8191
- lengths: int32 [2], replicated, may hold values from 256 to 1024
Outputs:
- hidden_out: bfloat16 [2, 1024, 4096], P(None, 'dp', 'vocab')
- token_logp: float32 [2, 1024], P(None, 'dp')
- mean_logp: float32 [], replicated
The draws below stay inside these ranges and needn't reach their ends.
Inputs may be any that keep to these rules, and one draw needn't show every extreme that they name: `head_w`: entries lie within 720 / sqrt(4096) of zero.
All inputs are finite; a program needn't handle non-finite values.
Results may differ from the reference program's by a relative error of at most 0.019.
Values may be sent and summed in bfloat16 or wider, within the bound.
A program may use at most 128 MiB of HBM per device.

```python
import math
import jax
import jax.numpy as jnp
from jax import lax

D = 4096
N = 16
R = 256
KCONV = 4
B = 2
L = 1024
E = 4096
V = 8192


def draw_head_w(key, part):
    values = jnp.clip(jax.random.normal(key, (V, D), jnp.float32), -6.0, 6.0) * (3.0 / math.sqrt(D))
    return values.astype(jnp.bfloat16)


def plant(entries, key, least, largest):
    spot = [jax.random.randint(jax.random.fold_in(key, axis), (), 0, length) for axis, length in enumerate(entries.shape)]
    main_axis = entries.shape.index(max(entries.shape))
    beside = spot[:main_axis] + [(spot[main_axis] + 1) % entries.shape[main_axis]] + spot[main_axis + 1:]
    return entries.at[tuple(spot)].set(least).at[tuple(beside)].set(largest)


def steps_of(key, extent, shards, low, largest):
    loudness, own = 1.0, jax.random.fold_in(key, 6)
    for position, shards_of in shards:
        steps = jnp.exp(jax.random.uniform(jax.random.fold_in(own, position), (shards_of,), jnp.float32, low / len(shards), largest / len(shards)))
        loudness = loudness * jnp.repeat(steps, extent[position] // shards_of).reshape([-1 if axis == position else 1 for axis in range(len(extent))])
    return loudness


def normal_values(key, extent, width, most, split=(), kind=jnp.bfloat16):
    array = jax.random.normal(key, extent, jnp.float32) * width
    if len(split) > 0:
        array = steps_of(key, extent, split, -0.22, 0.18) * array
    return jnp.clip(array, min=-most, max=most).astype(kind)


def setup_inputs(seed: int = 0) -> dict:
    keys = jax.random.split(jax.random.key(seed), 18)
    return {
        "resid": normal_values(keys[0], (B, L, D), 1.0, 6.0, ((1, 8),)),
        "norm_gain": jnp.clip(1.0 + 0.1 * jax.random.normal(keys[1], (D,), jnp.float32), 0.5, 1.5),
        "in_x": normal_values(keys[2], (D, E), D ** -0.5, 0.09375, ((0, 8), (1, 4))),
        "in_z": normal_values(keys[3], (D, E), D ** -0.5, 0.09375, ((0, 8), (1, 4))),
        "conv_w": normal_values(keys[4], (KCONV, E), 0.5, 3.0, ((1, 4),), jnp.float32),
        "conv_b": normal_values(keys[5], (E,), 0.5, 3.0, ((0, 4),), jnp.float32),
        "xdt_w": normal_values(keys[6], (E, R), E ** -0.5, 0.09375, ((0, 4),)),
        "xbc_w": normal_values(keys[7], (E, 2 * N), E ** -0.5, 0.09375, ((0, 4),)),
        "dt_gain": jnp.clip(1.0 + 0.1 * jax.random.normal(keys[8], (R,), jnp.float32), 0.5, 1.5),
        "dt_proj": normal_values(keys[9], (R, E), R ** -0.5, 0.375, ((1, 4),)),
        "dt_bias": jnp.clip(-4.0 + 5.0 * jax.random.uniform(keys[10], (E,), jnp.float32) ** steps_of(keys[10], (E,), ((0, 4),), -0.2, 0.2), -4.0, 1.0),
        "a_rate": jnp.clip(jnp.exp(math.log(1.0) - 9.2103404 * jax.random.uniform(keys[11], (E, N), jnp.float32) ** steps_of(keys[11], (E, N), ((0, 4),), -0.2, 0.2)), 0.0001, 1.0),
        "out_w": normal_values(keys[12], (E, D), E ** -0.5, 0.09375, ((0, 4),)),
        "final_gain": jnp.clip(1.0 + 0.1 * jax.random.normal(keys[13], (D,), jnp.float32), 0.5, 1.5),
        "head_w": draw_head_w(jax.random.fold_in(keys[17], 71), 0),
        "targets": plant(jax.random.randint(keys[15], (B, L), 0, V), jax.random.fold_in(keys[15], 1), 0, V - 1).astype(jnp.int32),
        "lengths": jax.random.randint(keys[16], (B,), L // 4, L + 1).astype(jnp.int32),
    }


def rms_norm(values, gain, epsilon):
    return values * lax.rsqrt(lax.optimization_barrier(jnp.mean(values * values, axis=-1, keepdims=True)) + epsilon) * gain

def reference(resid, norm_gain, in_x, in_z, conv_w, conv_b, xdt_w, xbc_w, dt_gain, dt_proj, dt_bias, a_rate, out_w, final_gain, head_w, targets, lengths):
    stream = resid.astype(jnp.float32)
    normed = rms_norm(stream, norm_gain, 1e-05).astype(jnp.bfloat16).reshape(B * L, D)
    x_inner = jnp.dot(normed, in_x, preferred_element_type=jnp.float32).astype(jnp.bfloat16).reshape(B, L, E)
    z_gate = jnp.dot(normed, in_z, preferred_element_type=jnp.float32).astype(jnp.bfloat16).reshape(B, L, E)
    padded = jnp.pad(x_inner.astype(jnp.float32), ((0, 0), (KCONV - 1, 0), (0, 0)))
    conv_sum = jnp.zeros((B, L, E), jnp.float32) + conv_b
    for tap_index in range(KCONV):
        conv_sum = conv_sum + conv_w[tap_index] * padded[:, tap_index:tap_index + L, :]
    conv_act = jax.nn.silu(conv_sum)
    conv_low = conv_act.astype(jnp.bfloat16).reshape(B * L, E)
    dt_raw = jnp.dot(conv_low, xdt_w, preferred_element_type=jnp.float32)
    bc_raw = jnp.dot(conv_low, xbc_w, preferred_element_type=jnp.float32)
    dt_normed = rms_norm(dt_raw, dt_gain, 1e-06).astype(jnp.bfloat16)
    step_size = jax.nn.softplus(jnp.dot(dt_normed, dt_proj, preferred_element_type=jnp.float32) + dt_bias).reshape(B, L, E)
    in_map = bc_raw[:, :N].reshape(B, L, N)
    out_map = bc_raw[:, N:].reshape(B, L, N)

    def advance(carry_state, inputs):
        step_now, conv_now, in_now, out_now = inputs
        carry_state = jnp.exp(-step_now[..., None] * a_rate) * carry_state + (step_now * conv_now)[..., None] * in_now[:, None, :]
        return (carry_state, lax.optimization_barrier(jnp.sum(carry_state * out_now[:, None, :], axis=-1)))
    start_state = jnp.zeros((B, E, N), jnp.float32)
    inputs = (step_size.transpose(1, 0, 2), conv_act.transpose(1, 0, 2), in_map.transpose(1, 0, 2), out_map.transpose(1, 0, 2))
    _, scanned = lax.scan(advance, start_state, inputs)
    mixed = scanned.transpose(1, 0, 2)
    gated = (mixed * jax.nn.silu(z_gate.astype(jnp.float32))).astype(jnp.bfloat16).reshape(B * L, E)
    mixer_out = jnp.dot(gated, out_w, preferred_element_type=jnp.float32)
    hidden = (stream.reshape(B * L, D) + mixer_out).astype(jnp.bfloat16)
    final = rms_norm(hidden.astype(jnp.float32), final_gain, 1e-05).astype(jnp.bfloat16)
    logits = lax.dot_general(final, head_w, (((1,), (1,)), ((), ())), preferred_element_type=jnp.float32)
    row_top = lax.optimization_barrier(jnp.max(logits, axis=-1))
    log_total = row_top + jnp.log(lax.optimization_barrier(jnp.sum(jnp.exp(logits - row_top[:, None]), axis=-1)))
    picked = jnp.take_along_axis(logits, targets.reshape(B * L, 1).astype(jnp.int32), axis=1)[:, 0]
    token_logp = (picked - log_total).reshape(B, L)
    valid_mask = jnp.arange(L, dtype=jnp.int32)[None, :] < lengths[:, None]
    mean_logp = jnp.sum(jnp.where(valid_mask, token_logp, 0.0)) / jnp.sum(lengths.astype(jnp.float32))
    return (hidden.reshape(B, L, D), token_logp, mean_logp)
```

```python
import functools

import jax
import jax.numpy as jnp
from jax import lax
from jax.experimental import pallas as pl
from jax.experimental.pallas import tpu as pltpu
from jax.sharding import PartitionSpec as P

MESH = pl.DeviceIdType.MESH
VMEM = pl.BlockSpec(memory_space=pltpu.VMEM)
CHUNKS = 8
LANE = 128


def peer(axis, shift):
    size = lax.axis_size(axis)
    return {axis: lax.rem(lax.axis_index(axis) + shift, size)}


def greet(axes):
    barrier = pltpu.get_barrier_semaphore()
    count = 0
    for axis in axes:
        for shift in range(1, lax.axis_size(axis)):
            pl.semaphore_signal(barrier, inc=1, device_id=peer(axis, shift), device_id_type=MESH)
            count += 1
    pl.semaphore_wait(barrier, count)


def remote(src, dst, send_sem, recv_sem, device):
    return pltpu.make_async_remote_copy(
        src_ref=src, dst_ref=dst, send_sem=send_sem, recv_sem=recv_sem,
        device_id=device, device_id_type=MESH,
    )


def call(kernel, out_shape, scratch, cid, cost_us, name):
    return pl.pallas_call(
        kernel,
        out_shape=out_shape,
        scratch_shapes=scratch,
        compiler_params=pltpu.CompilerParams(
            collective_id=cid, has_side_effects=True, vmem_limit_bytes=56 * 1024 * 1024
        ),
        cost_estimate=pl.CostEstimate(
            flops=0, bytes_accessed=int(cost_us * 3.0e6), transcendentals=0
        ),
        name=name,
    )


def dt_kernel(nv, ranks, part_ref, gain_ref, out_ref, recv, mine, s1, r1, s2, r2):
    me = lax.axis_index("vocab")
    rows = part_ref.shape[0] // nv
    greet(("vocab",))
    copies = []
    for shift in range(1, nv):
        target = lax.rem(me + shift, nv)
        copy = remote(
            part_ref.at[pl.ds(pl.multiple_of(target * rows, rows), rows)], recv.at[shift - 1],
            s1.at[shift - 1], r1.at[shift - 1], peer("vocab", shift),
        )
        copy.start()
        copies.append(copy)
    own = pl.ds(pl.multiple_of(me * rows, rows), rows)
    total = part_ref[own, :].astype(jnp.float32)
    for shift in range(1, nv):
        copies[shift - 1].wait()
        total = total + recv[shift - 1].astype(jnp.float32)
    dt = total[:, :ranks]
    scale = lax.rsqrt(jnp.mean(dt * dt, axis=-1, keepdims=True) + 1e-06)
    mine[:, :ranks] = (dt * scale * gain_ref[...]).astype(jnp.bfloat16)
    mine[:, ranks:] = total[:, ranks:].astype(jnp.bfloat16)
    copies = []
    for shift in range(1, nv):
        copy = remote(
            mine, out_ref.at[own], s2.at[shift - 1], r2.at[shift - 1], peer("vocab", shift)
        )
        copy.start()
        copies.append(copy)
    out_ref[own, :] = mine[...]
    for copy in copies:
        copy.wait()


def dt_reduce(part, gain, nv, ranks):
    rows, cols = part.shape
    sems = [pltpu.SemaphoreType.DMA((nv - 1,))] * 4
    return call(
        functools.partial(dt_kernel, nv, ranks),
        jax.ShapeDtypeStruct((rows, cols), jnp.bfloat16),
        [
            pltpu.VMEM((nv - 1, rows // nv, cols), jnp.bfloat16),
            pltpu.VMEM((rows // nv, cols), jnp.bfloat16),
        ] + sems,
        1, 10, "dt_reduce",
    )(part, gain)


def scan_kernel(
    nd, batch, nstate, ranks, low_ref, proj_ref, bias_ref, conv_ref, rate_ref, out_ref,
    step, drive, maps, result, state, sums, agg, tot, agg_in, tot_in, s1, r1, s2, r2,
):
    me = lax.axis_index("dp")
    rows, chans = conv_ref.shape
    lanes = chans // LANE
    length = rows // batch
    span = length // CHUNKS
    greet(("dp",))
    low_dt = low_ref[:, :ranks]
    maps[...] = low_ref[:, ranks:].astype(jnp.float32)
    wide = 2 if lanes % 2 == 0 else 1
    size = wide * LANE

    @pl.loop(0, lanes // wide)
    def _(g):
        cols = pl.ds(pl.multiple_of(g * size, size), size)
        raw = jnp.dot(
            low_dt, proj_ref[:, cols], preferred_element_type=jnp.float32
        ) + bias_ref[:, cols]
        value = jnp.maximum(raw, 0.0) + jnp.log1p(jnp.exp(-jnp.abs(raw)))
        pushed = value * conv_ref[:, cols]
        for w in range(wide):
            k = g * wide + w
            step[k] = value[:, w * LANE : (w + 1) * LANE]
            drive[k] = pushed[:, w * LANE : (w + 1) * LANE]

    def run(with_out):
        @pl.loop(0, lanes // wide)
        def _(g):
            for b in range(batch):
                rates = [
                    [
                        rate_ref[pl.ds(n, 1), pl.ds(pl.multiple_of((g * wide + w) * LANE, LANE), LANE)]
                        for n in range(nstate)
                    ]
                    for w in range(wide)
                ]

                def one(t, carry):
                    at = pl.ds(b * length + t, CHUNKS, stride=span)
                    both = maps[at, :]
                    held, extra = carry
                    held, extra = list(held), list(extra)
                    now = [step[g * wide + w, at, :] for w in range(wide)]
                    push = [drive[g * wide + w, at, :] for w in range(wide)]
                    acc = [None] * wide
                    for n in range(nstate):
                        into = jnp.broadcast_to(both[:, n : n + 1], (CHUNKS, LANE))
                        if with_out:
                            outof = jnp.broadcast_to(
                                both[:, nstate + n : nstate + n + 1], (CHUNKS, LANE)
                            )
                        for w in range(wide):
                            i = w * nstate + n
                            held[i] = (
                                jnp.exp(-now[w] * rates[w][n]) * held[i] + push[w] * into
                            )
                            if with_out:
                                term = held[i] * outof
                                acc[w] = term if acc[w] is None else acc[w] + term
                    for w in range(wide):
                        if with_out:
                            result[g * wide + w, at, :] = acc[w]
                        else:
                            extra[w] = extra[w] + now[w]
                    return tuple(held), tuple(extra)

                zero = jnp.zeros((CHUNKS, LANE), jnp.float32)
                if with_out:
                    first = tuple(
                        state[b, g * wide + w, pl.ds(n * CHUNKS, CHUNKS), :]
                        for w in range(wide) for n in range(nstate)
                    )
                    lax.fori_loop(0, span, one, (first, ()))
                else:
                    held, extra = lax.fori_loop(
                        0, span, one, ((zero,) * (wide * nstate), (zero,) * wide)
                    )
                    for w in range(wide):
                        for n in range(nstate):
                            state[b, g * wide + w, pl.ds(n * CHUNKS, CHUNKS), :] = held[
                                w * nstate + n
                            ]
                        sums[b, g * wide + w] = extra[w]

    run(False)

    @pl.loop(0, lanes)
    def _(k):
        cols = pl.ds(pl.multiple_of(k * LANE, LANE), LANE)
        rate = rate_ref[:, cols]
        for b in range(batch):
            carry = jnp.zeros((nstate, LANE), jnp.float32)
            for c in range(CHUNKS):
                part = state[b, k, pl.ds(c, nstate, stride=CHUNKS), :]
                carry = jnp.exp(-sums[b, k, pl.ds(c, 1), :] * rate) * carry + part
            agg[pl.ds(b * nstate, nstate), cols] = carry.astype(jnp.bfloat16)
            tot[pl.ds(b, 1), cols] = jnp.sum(sums[b, k], axis=0, keepdims=True)

    def pair(source, target):
        device = {"dp": target}
        return (
            remote(agg, agg_in.at[source], s1.at[target], r1.at[source], device),
            remote(tot, tot_in.at[source], s2.at[target], r2.at[source], device),
        )

    for other in range(nd):
        @pl.when(other > me)
        def _():
            for copy in pair(me, other):
                copy.start()

    for other in range(nd):
        @pl.when(other < me)
        def _():
            for copy in pair(other, me):
                copy.wait_recv()

    @pl.loop(0, lanes)
    def _(k):
        cols = pl.ds(pl.multiple_of(k * LANE, LANE), LANE)
        rate = rate_ref[:, cols]
        for b in range(batch):
            def earlier(d, carry):
                decay = jnp.exp(-tot_in[d, pl.ds(b, 1), cols] * rate)
                return decay * carry + agg_in[d, pl.ds(b * nstate, nstate), cols].astype(
                    jnp.float32
                )

            carry = lax.fori_loop(0, me, earlier, jnp.zeros((nstate, LANE), jnp.float32))
            for c in range(CHUNKS):
                at = pl.ds(c, nstate, stride=CHUNKS)
                part = state[b, k, at, :]
                state[b, k, at, :] = carry
                carry = jnp.exp(-sums[b, k, pl.ds(c, 1), :] * rate) * carry + part

    run(True)

    @pl.loop(0, lanes)
    def _(k):
        out_ref[:, pl.ds(pl.multiple_of(k * LANE, LANE), LANE)] = result[k]

    for other in range(nd):
        @pl.when(other > me)
        def _():
            for copy in pair(me, other):
                copy.wait_send()


def scan(low, proj, bias, conv, rate, batch, nd, ranks):
    rows, chans = conv.shape
    nstate = rate.shape[0]
    lanes = chans // LANE
    big = pltpu.VMEM((lanes, rows, LANE), jnp.float32)
    return call(
        functools.partial(scan_kernel, nd, batch, nstate, ranks),
        jax.ShapeDtypeStruct((rows, chans), jnp.float32),
        [
            big, big,
            pltpu.VMEM((rows, low.shape[1] - ranks), jnp.float32),
            big,
            pltpu.VMEM((batch, lanes, nstate * CHUNKS, LANE), jnp.float32),
            pltpu.VMEM((batch, lanes, CHUNKS, LANE), jnp.float32),
            pltpu.VMEM((batch * nstate, chans), jnp.bfloat16),
            pltpu.VMEM((batch, chans), jnp.float32),
            pltpu.VMEM((nd, batch * nstate, chans), jnp.bfloat16),
            pltpu.VMEM((nd, batch, chans), jnp.float32),
        ] + [pltpu.SemaphoreType.DMA((nd,))] * 4,
        2, 30, "scan",
    )(low, proj, bias, conv, rate)


def back_kernel(
    nv, nd, steps, relay_at, gated_ref, w_ref, resid_ref, gain_ref, head_ref, ids_ref, mask_ref,
    hidden_ref, logp_ref, sum_ref,
    weight, own, near, send_up, recv_up, send_down, recv_down, hid, fin, full, logits, ids, stats, heard,
    part, parts, w_sem, near_sem, up_s, up_r, down_s, down_r, gup_s, gup_r, gdown_s, gdown_r,
    fin_s, fin_r, ids_s, ids_r, head_l, head_s, head_r, pass_s, pass_r, stat_s, stat_r, sum_s, sum_r,
):
    me = lax.axis_index("vocab")
    dev = lax.axis_index("dp")
    chip, core = dev // 2, lax.rem(dev, 2)
    mate = {"dp": chip * 2 + 1 - core}
    above, below = {"vocab": lax.rem(me + 1, nv)}, {"vocab": lax.rem(me + nv - 1, nv)}
    rows, chans = gated_ref.shape
    width = w_ref.shape[1]
    share = width // nv
    entries, feats = head_ref.shape
    half = entries // 2
    size = rows // steps

    def block(index, length):
        return pl.ds(pl.multiple_of(index * length, length), length)

    weight_copies = []
    for s in range(nv):
        index = jnp.where(me * 2 < nv, nv - 1 - s, s)
        copy = pltpu.make_async_copy(
            w_ref.at[:, block(index, share)], weight.at[:, block(index, share)], w_sem.at[s]
        )
        copy.start()
        weight_copies.append((index, copy))
    near_copy = pltpu.make_async_copy(resid_ref.at[:, block(me, share)], near, near_sem)
    near_copy.start()
    greet_back(nv, nd)

    head_waits, head_sends, passes = gather_halves(
        nd, lambda c: head_ref.at[block(c, half)], lambda d: full.at[:, block(d, feats)], half,
        head_l, head_s, head_r, pass_s, pass_r,
    )
    mine = ids.at[core]
    ids[core] = ids_ref[...]
    ids_copy = remote(ids_ref, mine, ids_s, ids_r, mate)
    ids_copy.start()

    def up(i, j):
        return remote(send_up.at[i, j - 1], recv_up.at[i, j - 1], up_s.at[i, j - 1], up_r.at[i, j - 1], above)

    def down(i, j):
        return remote(send_down.at[i, j], recv_down.at[i, j], down_s.at[i, j], down_r.at[i, j], below)

    def spread_up(i, s):
        at = hid.at[block(i, size), block(s, share)]
        return remote(at, at, gup_s.at[i, s], gup_r.at[i, s], above)

    def spread_down(i, s):
        at = hid.at[block(i, size), block(s, share)]
        return remote(at, at, gdown_s.at[i, s - 1], gdown_r.at[i, s - 1], below)

    def fin_copy(i):
        at = fin.at[core, block(i, size)]
        return remote(at, at, fin_s.at[i], fin_r.at[i], mate)

    tile = min(512, share)
    for index, copy in weight_copies:
        copy.wait()

        @pl.loop(0, share // tile)
        def _(k):
            at = pl.ds(pl.multiple_of(index * share + k * tile, tile), tile)
            own[:, at] = jnp.dot(gated_ref[...], weight[:, at], preferred_element_type=jnp.float32)

        @pl.when((me == 0) & (index > 0))
        def _():
            @pl.loop(0, steps)
            def _(i):
                send_up[i, index - 1] = own[block(i, size), block(index, share)].astype(jnp.bfloat16)
                up(i, index).start()

        @pl.when((me == nv - 1) & (index < nv - 1))
        def _():
            @pl.loop(0, steps)
            def _(i):
                send_down[i, index] = own[block(i, size), block(index, share)].astype(jnp.bfloat16)
                down(i, index).start()

    near_copy.wait()

    def combine_up(i):
        for j in range(nv - 1, 0, -1):
            @pl.when((me > 0) & (me < j))
            def _():
                up(i, j).wait_recv()
                send_up[i, j - 1] = (
                    own[block(i, size), pl.ds(j * share, share)] + recv_up[i, j - 1].astype(jnp.float32)
                ).astype(jnp.bfloat16)
                up(i, j).start()

    def combine_down(i):
        for j in range(nv - 1):
            @pl.when((me < nv - 1) & (me > j))
            def _():
                down(i, j).wait_recv()
                send_down[i, j] = (
                    own[block(i, size), pl.ds(j * share, share)] + recv_down[i, j].astype(jnp.float32)
                ).astype(jnp.bfloat16)
                down(i, j).start()

    def finish(i):
        at = block(i, size)
        own[at, block(me, share)] = own[at, block(me, share)] + near[at, :].astype(jnp.float32)

        @pl.when(me > 0)
        def _():
            up(i, me).wait_recv()
            own[at, block(me, share)] = own[at, block(me, share)] + recv_up[i, me - 1].astype(jnp.float32)

        @pl.when(me < nv - 1)
        def _():
            down(i, me).wait_recv()
            own[at, block(me, share)] = own[at, block(me, share)] + recv_down[i, me].astype(jnp.float32)

        value = own[at, block(me, share)].astype(jnp.bfloat16)
        hidden_ref[at, :] = value
        hid[at, block(me, share)] = value

        @pl.when(me < nv - 1)
        def _():
            spread_up(i, me).start()

        @pl.when(me > 0)
        def _():
            spread_down(i, me).start()

    def forward(i, hops):
        low, high = me - hops, me + hops

        @pl.when(low >= 0)
        def _():
            spread_up(i, low).wait_recv()

            @pl.when(me < nv - 1)
            def _():
                spread_up(i, low).start()

        @pl.when(high < nv)
        def _():
            spread_down(i, high).wait_recv()

            @pl.when(me > 0)
            def _():
                spread_down(i, high).start()

    def normalize(i):
        at = block(i, size)
        wide = hid[at, :].astype(jnp.float32)
        scale = lax.rsqrt(jnp.mean(wide * wide, axis=-1, keepdims=True) + 1e-05)
        fin[core, at] = (wide * scale * gain_ref[...]).astype(jnp.bfloat16)
        fin_copy(i).start()

    late = jnp.where(me * 2 >= nv, 1, 0)

    def walk(first, last):
        @pl.loop(first, last)
        def _(t):
            def at(i, step):
                @pl.when((i >= 0) & (i < steps))
                def _():
                    step(i)

            at(t - late, combine_up)
            at(t - 1 + late, combine_down)
            at(t - 2, finish)
            for hops in range(1, nv):
                at(t - 2 - hops, functools.partial(forward, hops=hops))
            at(t - 1 - nv, normalize)

    walk(0, relay_at)
    passes()
    walk(relay_at, steps + nv + 1)

    @pl.loop(0, steps)
    def _(i):
        remote(
            fin.at[core, block(i, size)], fin.at[1 - core, block(i, size)], fin_s.at[i], fin_r.at[i], mate
        ).wait_recv()
    ids_copy.wait()
    head_waits()

    vt = min(256, half)
    for s in range(2):
        @pl.loop(0, half // vt)
        def _(k):
            logits[block(k, vt), s * rows : (s + 1) * rows] = lax.dot_general(
                full[block(k, vt), :], fin[s], (((1,), (1,)), ((), ())), preferred_element_type=jnp.float32
            )

        def highest(k, top):
            return jnp.maximum(
                top, jnp.max(logits[block(k, vt), s * rows : (s + 1) * rows], axis=0, keepdims=True)
            )

        top = lax.fori_loop(0, half // vt, highest, jnp.full((1, rows), -jnp.inf, jnp.float32))
        wanted = ids[s, 0:1, :] - (me * entries + core * half)

        def gather(k, carry):
            total, picked = carry
            values = logits[block(k, vt), s * rows : (s + 1) * rows]
            entry = lax.broadcasted_iota(jnp.int32, values.shape, 0) + k * vt
            total = total + jnp.sum(jnp.exp(values - top), axis=0, keepdims=True)
            picked = picked + jnp.sum(jnp.where(entry == wanted, values, 0.0), axis=0, keepdims=True)
            return total, picked

        zero = jnp.zeros((1, rows), jnp.float32)
        total, picked = lax.fori_loop(0, half // vt, gather, (zero, zero))
        stats[s, 0:1, :] = top
        stats[s, 1:2, :] = total
        stats[s, 2:3, :] = picked
        stats[s, 3:8, :] = jnp.zeros((5, rows), jnp.float32)

    sends = []
    for shift in range(nv):
        for other in range(2):
            if shift == 0 and other == 0:
                continue
            owner = core if other == 0 else 1 - core
            copy = remote(
                stats.at[owner], heard.at[me, core], stat_s.at[shift, other], stat_r.at[me, core],
                {"vocab": lax.rem(me + shift, nv), "dp": chip * 2 + owner},
            )
            copy.start()
            sends.append(copy)
    heard[me, core] = stats[core]
    for z in range(nv):
        for c in range(2):
            @pl.when((z != me) | (c != core))
            def _():
                remote(stats.at[0], heard.at[z, c], stat_s.at[0, 1], stat_r.at[z, c], mate).wait_recv()
    everyone = [heard[z, c] for z in range(nv) for c in range(2)]
    top = everyone[0][0:1]
    for one in everyone[1:]:
        top = jnp.maximum(top, one[0:1])
    total = jnp.zeros_like(top)
    picked = jnp.zeros_like(top)
    for one in everyone:
        total = total + one[1:2] * jnp.exp(one[0:1] - top)
        picked = picked + one[2:3]
    logp = picked - (top + jnp.log(total))
    logp_ref[...] = logp
    masked = jnp.sum(jnp.where(mask_ref[...] > 0.0, logp, 0.0), axis=-1, keepdims=True)
    part[...] = jnp.broadcast_to(masked, part.shape)
    for shift in range(1, nd):
        copy = remote(
            part, parts.at[dev], sum_s.at[shift - 1], sum_r.at[dev], {"dp": lax.rem(dev + shift, nd)}
        )
        copy.start()
        sends.append(copy)
    parts[dev] = part[...]
    for d in range(nd):
        @pl.when(d != dev)
        def _():
            remote(part, parts.at[d], sum_s.at[0], sum_r.at[d], mate).wait_recv()
    grand = parts[0]
    for d in range(1, nd):
        grand = grand + parts[d]
    sum_ref[...] = grand

    for copy in sends:
        copy.wait_send()
    head_sends()

    @pl.loop(0, steps)
    def _(i):
        fin_copy(i).wait_send()
        for j in range(1, nv):
            @pl.when(me < j)
            def _():
                up(i, j).wait_send()
        for j in range(nv - 1):
            @pl.when(me > j)
            def _():
                down(i, j).wait_send()
        for s in range(nv - 1):
            @pl.when((me >= s) & (me < nv - 1))
            def _():
                spread_up(i, s).wait_send()
        for s in range(1, nv):
            @pl.when((me <= s) & (me > 0))
            def _():
                spread_down(i, s).wait_send()


def greet_back(nv, nd):
    barrier = pltpu.get_barrier_semaphore()
    me, dev = lax.axis_index("vocab"), lax.axis_index("dp")
    mate = dev // 2 * 2 + 1 - lax.rem(dev, 2)
    for shift in range(1, nd):
        pl.semaphore_signal(barrier, inc=1, device_id=peer("dp", shift), device_id_type=MESH)
    for shift in range(1, nv):
        z = lax.rem(me + shift, nv)
        pl.semaphore_signal(barrier, inc=1, device_id={"vocab": z}, device_id_type=MESH)
        pl.semaphore_signal(barrier, inc=1, device_id={"vocab": z, "dp": mate}, device_id_type=MESH)
    pl.semaphore_wait(barrier, nd - 1 + 2 * (nv - 1))


def gather_halves(nd, source, target, length, local, send, recv, pass_s, pass_r):
    dev = lax.axis_index("dp")
    chip, core = dev // 2, lax.rem(dev, 2)
    keep = pltpu.make_async_copy(source(core), target(dev), local)
    keep.start()
    copies = [remote(source(1 - core), target(dev), send.at[0, 0], recv.at[0, core], {"dp": chip * 2 + 1 - core})]
    copies[0].start()
    waits = [remote(source(0), target(chip * 2 + 1 - core), send.at[0, 0], recv.at[0, 1 - core], {"dp": dev})]
    if nd != 8:
        for shift in range(1, nd // 2):
            there = lax.rem(chip + shift, nd // 2)
            back = lax.rem(chip + nd // 2 - shift, nd // 2)
            for c in range(2):
                copy = remote(
                    source(c), target(dev), send.at[shift, c], recv.at[shift, core], {"dp": there * 2 + c}
                )
                copy.start()
                copies.append(copy)
                waits.append(
                    remote(source(c), target(back * 2 + c), send.at[shift, c], recv.at[shift, c], {"dp": dev})
                )
        passes = lambda: None
    else:
        piece = length // 2
        sides = (chip + 1 - 2 * lax.rem(chip, 2), lax.rem(chip + 2, 4))

        def at(ref, p):
            return ref.at[pl.ds(p * piece, piece)]

        first = []
        for turn in range(2):
            for side in range(2):
                p = side if turn == 0 else 1 - side
                for c in range(2):
                    k = 1 + side * 2 + p
                    copy = remote(
                        at(source(c), p), at(target(dev), p), send.at[k, c], recv.at[k, core],
                        {"dp": sides[side] * 2 + c},
                    )
                    copy.start()
                    copies.append(copy)
                    came = at(target(sides[side] * 2 + c), p)
                    wait = remote(came, came, send.at[k, c], recv.at[k, c], {"dp": dev})
                    if turn == 0:
                        first.append((side, p, c, wait, came))
                    else:
                        waits.append(wait)

        far = 3 - chip
        for side in range(2):
            for c in range(2):
                came = at(target(far * 2 + c), 1 - side)
                waits.append(
                    remote(came, came, pass_s.at[side, c], pass_r.at[1 - side, c], {"dp": dev})
                )

        def passes():
            for side, p, c, wait, came in first:
                wait.wait_recv()
                copy = remote(
                    came, came, pass_s.at[side, c], pass_r.at[p, c], {"dp": sides[1 - side] * 2 + core}
                )
                copy.start()
                copies.append(copy)

    def finish_waits():
        keep.wait()
        for wait in waits:
            wait.wait_recv()

    def finish_sends():
        for copy in copies:
            copy.wait_send()

    return finish_waits, finish_sends, passes


def back(gated, w, resid, gain, head, ids, mask, nv, nd, steps=4, relay_at=3):
    rows, chans = gated.shape
    width = w.shape[1]
    share = width // nv
    half = head.shape[0] // 2
    size = rows // steps
    dma = pltpu.SemaphoreType.DMA
    line = pltpu.VMEM((steps, nv - 1, size, share), jnp.bfloat16)
    lanes = 5 if nd == 8 else nd // 2
    anywhere = pl.BlockSpec(memory_space=pl.ANY)
    return pl.pallas_call(
        functools.partial(back_kernel, nv, nd, steps, relay_at),
        out_shape=(
            jax.ShapeDtypeStruct((rows, share), jnp.bfloat16),
            jax.ShapeDtypeStruct((1, rows), jnp.float32),
            jax.ShapeDtypeStruct((8, LANE), jnp.float32),
        ),
        in_specs=[VMEM, anywhere, anywhere, VMEM, anywhere, VMEM, VMEM],
        out_specs=(VMEM, VMEM, VMEM),
        scratch_shapes=[
            pltpu.VMEM((chans, width), jnp.bfloat16),
            pltpu.VMEM((rows, width), jnp.float32),
            pltpu.VMEM((rows, share), jnp.bfloat16),
            line, line, line, line,
            pltpu.VMEM((rows, width), jnp.bfloat16),
            pltpu.VMEM((2, rows, width), jnp.bfloat16),
            pltpu.VMEM((half, width), jnp.bfloat16),
            pltpu.VMEM((half, 2 * rows), jnp.float32),
            pltpu.VMEM((2, 8, rows), jnp.int32),
            pltpu.VMEM((2, 8, rows), jnp.float32),
            pltpu.VMEM((nv, 2, 8, rows), jnp.float32),
            pltpu.VMEM((8, LANE), jnp.float32),
            pltpu.VMEM((nd, 8, LANE), jnp.float32),
            dma((nv,)), dma,
        ] + [dma((steps, nv - 1))] * 8 + [
            dma((steps,)), dma((steps,)), dma, dma, dma, dma((lanes, 2)), dma((lanes, 2)),
            dma((2, 2)), dma((2, 2)), dma((nv, 2)), dma((nv, 2)), dma((nd,)), dma((nd,)),
        ],
        compiler_params=pltpu.CompilerParams(
            collective_id=3, has_side_effects=True, vmem_limit_bytes=60 * 1024 * 1024
        ),
        cost_estimate=pl.CostEstimate(flops=0, bytes_accessed=int(80 * 3.0e6), transcendentals=0),
        name="back",
    )(gated, w, resid, gain, head, ids, mask)


def rms_norm(values, gain, epsilon):
    return values * lax.rsqrt(jnp.mean(values * values, axis=-1, keepdims=True) + epsilon) * gain


def body(
    resid, norm_gain, in_x, in_z, conv_w, conv_b, xdt_w, xbc_w, dt_gain, dt_proj, dt_bias,
    a_rate, out_w, final_gain, head_w, targets, lengths,
):
    nv, nd = lax.axis_size("vocab"), lax.axis_size("dp")
    batch, local_len, width = resid.shape
    channels = in_x.shape[1]
    nstate = a_rate.shape[1]
    ranks = xdt_w.shape[1]
    kernel_len = conv_w.shape[0]
    rows = batch * local_len

    full_x = lax.all_gather(in_x, "dp", axis=0, tiled=True)
    in_z, _ = lax.optimization_barrier((in_z, in_x))
    full_z = lax.all_gather(in_z, "dp", axis=0, tiled=True)

    pad = -(2 * nstate) % 128
    low_w = jnp.concatenate([xdt_w, xbc_w, jnp.zeros((channels, pad), jnp.bfloat16)], axis=1)
    flat = resid.reshape(rows, width)
    stream = flat.astype(jnp.float32)
    normed = rms_norm(stream, norm_gain, 1e-05).astype(jnp.bfloat16)
    x_inner = (
        jnp.dot(normed, full_x, preferred_element_type=jnp.float32)
        .astype(jnp.bfloat16)
        .reshape(batch, local_len, channels)
    )
    before = lax.ppermute(
        x_inner[:, local_len - (kernel_len - 1) :, :], "dp", [(i, i + 1) for i in range(nd - 1)]
    )
    padded = jnp.concatenate([before, x_inner], axis=1).astype(jnp.float32)
    conv_sum = jnp.zeros((batch, local_len, channels), jnp.float32) + conv_b
    for tap in range(kernel_len):
        conv_sum = conv_sum + conv_w[tap] * padded[:, tap : tap + local_len, :]
    conv_act = jax.nn.silu(conv_sum).reshape(rows, channels)
    part = jnp.dot(
        conv_act.astype(jnp.bfloat16), low_w, preferred_element_type=jnp.float32
    ).astype(jnp.bfloat16)
    low = dt_reduce(part, dt_gain[None, :], nv, ranks)
    mixed = scan(low, dt_proj, dt_bias[None, :], conv_act, a_rate.T, batch, nd, ranks)
    z_gate = (
        jnp.dot(normed, full_z, preferred_element_type=jnp.float32)
        .astype(jnp.bfloat16)
        .astype(jnp.float32)
    )
    gated = (mixed * jax.nn.silu(z_gate)).astype(jnp.bfloat16)
    share = width // nv
    positions = lax.axis_index("dp") * local_len + jnp.arange(local_len, dtype=jnp.int32)
    mask = (positions[None, :] < lengths[:, None]).astype(jnp.float32).reshape(1, rows)
    ids = jnp.broadcast_to(targets.reshape(1, rows), (8, rows))
    hidden_share, logp, grand = back(gated, out_w, flat, final_gain[None, :], head_w, ids, mask, nv, nd)
    mean_logp = grand[0, 0] / jnp.sum(lengths.astype(jnp.float32))
    return (
        hidden_share.reshape(batch, local_len, share),
        logp.reshape(batch, local_len),
        mean_logp,
    )


def solution(mesh):
    in_specs = (
        P(None, "dp", None), P(), P("dp", "vocab"), P("dp", "vocab"), P(None, "vocab"), P("vocab"),
        P("vocab", None), P("vocab", None), P(), P(None, "vocab"), P("vocab"), P("vocab", None),
        P("vocab", None), P(), P("vocab", "dp"), P(None, "dp"), P(),
    )
    out_specs = (P(None, "dp", "vocab"), P(None, "dp"), P())
    return jax.shard_map(body, mesh=mesh, in_specs=in_specs, out_specs=out_specs, check_vma=False)
```

```python
import functools

import jax
import jax.numpy as jnp
from jax import lax
from jax.experimental import pallas as pl
from jax.experimental.pallas import tpu as pltpu
from jax.sharding import PartitionSpec as P

MESH = pl.DeviceIdType.MESH
VMEM = pl.BlockSpec(memory_space=pltpu.VMEM)
CHUNKS = 8
LANE = 128


def peer(axis, shift):
    size = lax.axis_size(axis)
    return {axis: lax.rem(lax.axis_index(axis) + shift, size)}


def greet(axes):
    barrier = pltpu.get_barrier_semaphore()
    count = 0
    for axis in axes:
        for shift in range(1, lax.axis_size(axis)):
            pl.semaphore_signal(barrier, inc=1, device_id=peer(axis, shift), device_id_type=MESH)
            count += 1
    pl.semaphore_wait(barrier, count)


def remote(src, dst, send_sem, recv_sem, device):
    return pltpu.make_async_remote_copy(
        src_ref=src, dst_ref=dst, send_sem=send_sem, recv_sem=recv_sem,
        device_id=device, device_id_type=MESH,
    )


def front_kernel(
    nv, nd, batch, ranks, nstate, resid_ref, gain_ref, in_x_ref, in_z_ref, conv_w_ref, conv_b_ref, low_w_ref,
    dt_gain_ref, proj_ref, bias_ref, rate_ref, gated_ref,
    normed, full_x, full_z, made, whole, zwhole, edge, padded, act, part, low_recv, low_mine, low,
    step, drive, maps, result, decay, spread, state, sums, agg, tot, agg_in, tot_in,
    norm_s, norm_r, x_l, x_s, x_r, xp_s, xp_r, z_l, z_s, z_r, zp_s, zp_r,
    swap_s, swap_r, edge_s, edge_r, zswap_s, zswap_r, l1_s, l1_r, l2_s, l2_r, s1, r1, s2, r2,
):
    me = lax.axis_index("dp")
    chip, core = me // 2, lax.rem(me, 2)
    mate = {"dp": chip * 2 + 1 - core}
    vme = lax.axis_index("vocab")
    rows, width = resid_ref.shape
    feats, chans = in_x_ref.shape
    half = chans // 2
    length = rows // batch
    greet(("dp", "vocab"))

    def columns(c):
        return pl.ds(pl.multiple_of(c * half, half), half)

    def block(index, size):
        return pl.ds(pl.multiple_of(index * size, size), size)

    x_waits, x_sends, x_passes = gather_halves(
        nd, lambda c: in_x_ref.at[:, columns(c)], lambda d: full_x.at[block(d, feats)], feats,
        x_l, x_s, x_r, xp_s, xp_r,
    )
    piece = min(32, rows)

    @pl.loop(0, rows // piece)
    def _(i):
        at = block(i, piece)
        wide = resid_ref[at, :].astype(jnp.float32)
        scale = lax.rsqrt(jnp.mean(wide * wide, axis=-1, keepdims=True) + 1e-05)
        normed[core, at] = (wide * scale * gain_ref[...]).astype(jnp.bfloat16)

    norm_copy = remote(normed.at[core], normed.at[core], norm_s, norm_r, mate)
    norm_copy.start()
    remote(normed.at[core], normed.at[1 - core], norm_s, norm_r, mate).wait_recv()
    x_passes()
    x_waits()
    tile = min(256, half)

    def project(full, r):
        @pl.loop(0, half // tile)
        def _(k):
            value = jnp.dot(normed[r], full[:, block(k, tile)], preferred_element_type=jnp.float32)
            made[r, :, :, block(k, tile)] = value.astype(jnp.bfloat16).reshape(batch, length, tile)

    def swap(send, recv):
        return remote(made.at[1 - core], whole.at[:, :, columns(core)], send, recv, mate)

    def swapped(send, recv):
        return remote(made.at[core], whole.at[:, :, columns(1 - core)], send, recv, mate)

    def zswap(send, recv):
        return remote(made.at[1 - core], zwhole.at[:, :, columns(core)], send, recv, mate)

    def zswapped(send, recv):
        return remote(made.at[core], zwhole.at[:, :, columns(1 - core)], send, recv, mate)

    project(full_x, 1 - core)
    swap(swap_s, swap_r).start()
    project(full_x, core)
    whole[:, :, columns(core)] = made[core]
    last = length - 16

    def tail_of(r):
        return made.at[r, :, pl.ds(last, 16), :]

    def tail_at(c):
        return edge.at[:, :, columns(c)]

    onward = {"dp": lax.rem(chip + 1, nd // 2) * 2}
    across = {"dp": chip * 2 + 1}

    @pl.when(core == 0)
    def _():
        remote(tail_of(0), tail_at(core), edge_s.at[0], edge_r.at[core], across).start()

    @pl.when(core == 1)
    def _():
        edge[:, :, columns(core)] = made[0, :, pl.ds(last, 16), :]

    @pl.when(chip < nd // 2 - 1)
    def _():
        remote(tail_of(1), tail_at(core), edge_s.at[1], edge_r.at[core], onward).start()

    z_waits, z_sends, z_passes = gather_halves(
        nd, lambda c: in_z_ref.at[:, columns(c)], lambda d: full_z.at[block(d, feats)], feats,
        z_l, z_s, z_r, zp_s, zp_r,
    )

    @pl.when(me == 0)
    def _():
        edge[...] = jnp.zeros_like(edge)

    swapped(swap_s, swap_r).wait_recv()
    swap(swap_s, swap_r).wait_send()

    @pl.when(core == 1)
    def _():
        remote(tail_of(0), tail_at(0), edge_s.at[0], edge_r.at[0], mate).wait_recv()

    @pl.when((core == 0) & (chip > 0))
    def _():
        for c in range(2):
            remote(tail_of(1), tail_at(c), edge_s.at[1], edge_r.at[c], mate).wait_recv()

    taps = conv_w_ref.shape[0]
    lane = min(256, chans)

    @pl.loop(0, chans // lane)
    def _(k):
        cols = block(k, lane)
        for b in range(batch):
            padded[0:8, :] = edge[b, 8:16, cols].astype(jnp.float32)
            padded[8:, :] = whole[b, :, cols].astype(jnp.float32)
            total = jnp.zeros((length, lane), jnp.float32) + conv_b_ref[:, cols]
            for tap in range(taps):
                first = 8 - (taps - 1) + tap
                total = total + conv_w_ref[tap : tap + 1, cols] * padded[first : first + length, :]
            act[b * length : (b + 1) * length, cols] = total / (1.0 + jnp.exp(-total))

    part[...] = jnp.dot(
        act[...].astype(jnp.bfloat16), low_w_ref[...], preferred_element_type=jnp.float32
    ).astype(jnp.bfloat16)

    share = rows // nv
    copies = []
    for shift in range(1, nv):
        target = lax.rem(vme + shift, nv)
        copy = remote(
            part.at[block(target, share)], low_recv.at[shift - 1],
            l1_s.at[shift - 1], l1_r.at[shift - 1], peer("vocab", shift),
        )
        copy.start()
        copies.append(copy)
    own = block(vme, share)
    total = part[own, :].astype(jnp.float32)
    for shift in range(1, nv):
        copies[shift - 1].wait()
        total = total + low_recv[shift - 1].astype(jnp.float32)
    dt = total[:, :ranks]
    scale = lax.rsqrt(jnp.mean(dt * dt, axis=-1, keepdims=True) + 1e-06)
    low_mine[:, :ranks] = (dt * scale * dt_gain_ref[...]).astype(jnp.bfloat16)
    low_mine[:, ranks:] = total[:, ranks:].astype(jnp.bfloat16)
    copies = []
    for shift in range(1, nv):
        copy = remote(low_mine, low.at[own], l2_s.at[shift - 1], l2_r.at[shift - 1], peer("vocab", shift))
        copy.start()
        copies.append(copy)
    low[own, :] = low_mine[...]
    for copy in copies:
        copy.wait()

    lanes = chans // LANE
    span = length // CHUNKS
    low_dt = low[:, :ranks]
    maps[...] = low[:, ranks:].astype(jnp.float32)
    wide = 2 if lanes % 2 == 0 else 1
    size = wide * LANE

    @pl.loop(0, lanes // wide)
    def _(g):
        cols = pl.ds(pl.multiple_of(g * size, size), size)
        raw = jnp.dot(
            low_dt, proj_ref[:, cols], preferred_element_type=jnp.float32
        ) + bias_ref[:, cols]
        value = jnp.maximum(raw, 0.0) + jnp.log1p(jnp.exp(-jnp.abs(raw)))
        pushed = value * act[:, cols]
        for w in range(wide):
            k = g * wide + w
            step[k] = value[:, w * LANE : (w + 1) * LANE]
            drive[k] = pushed[:, w * LANE : (w + 1) * LANE]

    for n in range(2 * nstate):
        spread[n] = jnp.broadcast_to(maps[:, n : n + 1], (rows, LANE))

    def local_scan(group):
        @pl.loop(0, lanes // group)
        def _(g):
            for b in range(batch):
                rates = [
                    [
                        rate_ref[pl.ds(n, 1), pl.ds(pl.multiple_of((g * group + w) * LANE, LANE), LANE)]
                        for n in range(nstate)
                    ]
                    for w in range(group)
                ]

                def one(t, carry):
                    at = pl.ds(b * length + t, CHUNKS, stride=span)
                    held, extra = carry
                    held, extra = list(held), list(extra)
                    now = [step[g * group + w, at, :] for w in range(group)]
                    push = [drive[g * group + w, at, :] for w in range(group)]
                    for n in range(nstate):
                        into = spread[n, at, :]
                        for w in range(group):
                            i = w * nstate + n
                            factor = jnp.exp(-now[w] * rates[w][n])
                            decay[b * span + t, g * group + w, pl.ds(n * CHUNKS, CHUNKS), :] = factor
                            held[i] = factor * held[i] + push[w] * into
                    for w in range(group):
                        extra[w] = extra[w] + now[w]
                    return tuple(held), tuple(extra)

                zero = jnp.zeros((CHUNKS, LANE), jnp.float32)
                held, extra = lax.fori_loop(0, span, one, ((zero,) * (group * nstate), (zero,) * group))
                for w in range(group):
                    for n in range(nstate):
                        state[b, g * group + w, pl.ds(n * CHUNKS, CHUNKS), :] = held[w * nstate + n]
                    sums[b, g * group + w] = extra[w]

    def final_scan(group):
        @pl.loop(0, lanes // group)
        def _(g):
            for b in range(batch):
                def one(t, carry):
                    at = pl.ds(b * length + t, CHUNKS, stride=span)
                    held = list(carry)
                    push = [drive[g * group + w, at, :] for w in range(group)]
                    acc = [None] * group
                    for n in range(nstate):
                        into = spread[n, at, :]
                        outof = spread[nstate + n, at, :]
                        for w in range(group):
                            i = w * nstate + n
                            factor = decay[b * span + t, g * group + w, pl.ds(n * CHUNKS, CHUNKS), :]
                            held[i] = factor * held[i] + push[w] * into
                            term = held[i] * outof
                            acc[w] = term if acc[w] is None else acc[w] + term
                    for w in range(group):
                        result[g * group + w, at, :] = acc[w]
                    return tuple(held)

                lax.fori_loop(
                    0, span, one,
                    tuple(
                        state[b, g * group + w, pl.ds(n * CHUNKS, CHUNKS), :]
                        for w in range(group) for n in range(nstate)
                    ),
                )

    local_scan(2 if lanes % 2 == 0 else 1)

    @pl.loop(0, lanes)
    def _(k):
        cols = pl.ds(pl.multiple_of(k * LANE, LANE), LANE)
        rate = rate_ref[:, cols]
        for b in range(batch):
            carry = jnp.zeros((nstate, LANE), jnp.float32)
            for c in range(CHUNKS):
                part = state[b, k, pl.ds(c, nstate, stride=CHUNKS), :]
                carry = jnp.exp(-sums[b, k, pl.ds(c, 1), :] * rate) * carry + part
            agg[pl.ds(b * nstate, nstate), cols] = carry.astype(jnp.bfloat16)
            tot[pl.ds(b, 1), cols] = jnp.sum(sums[b, k], axis=0, keepdims=True)

    def pair(source, target):
        device = {"dp": target}
        return (
            remote(agg, agg_in.at[source], s1.at[target], r1.at[source], device),
            remote(tot, tot_in.at[source], s2.at[target], r2.at[source], device),
        )

    for other in range(nd):
        @pl.when(other > me)
        def _():
            for copy in pair(me, other):
                copy.start()

    for other in range(nd):
        @pl.when(other < me)
        def _():
            for copy in pair(other, me):
                copy.wait_recv()

    @pl.loop(0, lanes)
    def _(k):
        cols = pl.ds(pl.multiple_of(k * LANE, LANE), LANE)
        rate = rate_ref[:, cols]
        for b in range(batch):
            def earlier(d, carry):
                decay = jnp.exp(-tot_in[d, pl.ds(b, 1), cols] * rate)
                return decay * carry + agg_in[d, pl.ds(b * nstate, nstate), cols].astype(
                    jnp.float32
                )

            carry = lax.fori_loop(0, me, earlier, jnp.zeros((nstate, LANE), jnp.float32))
            for c in range(CHUNKS):
                at = pl.ds(c, nstate, stride=CHUNKS)
                part = state[b, k, at, :]
                state[b, k, at, :] = carry
                carry = jnp.exp(-sums[b, k, pl.ds(c, 1), :] * rate) * carry + part

    z_passes()
    final_scan(2 if lanes % 2 == 0 else 1)

    @pl.when(core == 0)
    def _():
        remote(tail_of(0), tail_at(core), edge_s.at[0], edge_r.at[core], across).wait_send()

    @pl.when(chip < nd // 2 - 1)
    def _():
        remote(tail_of(1), tail_at(core), edge_s.at[1], edge_r.at[core], onward).wait_send()

    z_waits()
    project(full_z, 1 - core)
    zswap(zswap_s, zswap_r).start()
    project(full_z, core)
    zwhole[:, :, columns(core)] = made[core]
    zswapped(zswap_s, zswap_r).wait_recv()

    @pl.loop(0, lanes)
    def _(k):
        cols = block(k, LANE)
        for b in range(batch):
            gate = zwhole[b, :, cols].astype(jnp.float32)
            at = pl.ds(b * length, length)
            gated_ref[at, cols] = (result[k, at] * (gate / (1.0 + jnp.exp(-gate)))).astype(jnp.bfloat16)

    for other in range(nd):
        @pl.when(other > me)
        def _():
            for copy in pair(me, other):
                copy.wait_send()
    norm_copy.wait_send()
    zswap(zswap_s, zswap_r).wait_send()
    x_sends()
    z_sends()


def front(resid, gain, in_x, in_z, conv_w, conv_b, low_w, dt_gain, proj, bias, rate, batch, nv, nd):
    rows, width = resid.shape
    chans = in_x.shape[1]
    half = chans // 2
    ranks = proj.shape[0]
    nstate = rate.shape[0]
    lanes = chans // LANE
    length = rows // batch
    cols = low_w.shape[1]
    dma = pltpu.SemaphoreType.DMA
    big = pltpu.VMEM((lanes, rows, LANE), jnp.float32)
    slots = 5 if nd == 8 else nd // 2
    gathers = [dma, dma((slots, 2)), dma((slots, 2)), dma((2, 2)), dma((2, 2))]
    anywhere = pl.BlockSpec(memory_space=pl.ANY)
    return pl.pallas_call(
        functools.partial(front_kernel, nv, nd, batch, ranks, nstate),
        out_shape=jax.ShapeDtypeStruct((rows, chans), jnp.bfloat16),
        in_specs=[VMEM, VMEM, anywhere, anywhere] + [VMEM] * 7,
        out_specs=VMEM,
        scratch_shapes=[
            pltpu.VMEM((2, rows, width), jnp.bfloat16),
            pltpu.VMEM((width, half), jnp.bfloat16),
            pltpu.VMEM((width, half), jnp.bfloat16),
            pltpu.VMEM((2, batch, length, half), jnp.bfloat16),
            pltpu.VMEM((batch, length, chans), jnp.bfloat16),
            pltpu.VMEM((batch, length, chans), jnp.bfloat16),
            pltpu.VMEM((batch, 16, chans), jnp.bfloat16),
            pltpu.VMEM((length + 8, min(256, chans)), jnp.float32),
            pltpu.VMEM((rows, chans), jnp.float32),
            pltpu.VMEM((rows, cols), jnp.bfloat16),
            pltpu.VMEM((nv - 1, rows // nv, cols), jnp.bfloat16),
            pltpu.VMEM((rows // nv, cols), jnp.bfloat16),
            pltpu.VMEM((rows, cols), jnp.bfloat16),
            big, big,
            pltpu.VMEM((rows, cols - ranks), jnp.float32),
            big,
            pltpu.VMEM((rows // CHUNKS, lanes, nstate * CHUNKS, LANE), jnp.float32),
            pltpu.VMEM((2 * nstate, rows, LANE), jnp.float32),
            pltpu.VMEM((batch, lanes, nstate * CHUNKS, LANE), jnp.float32),
            pltpu.VMEM((batch, lanes, CHUNKS, LANE), jnp.float32),
            pltpu.VMEM((batch * nstate, chans), jnp.bfloat16),
            pltpu.VMEM((batch, chans), jnp.float32),
            pltpu.VMEM((nd, batch * nstate, chans), jnp.bfloat16),
            pltpu.VMEM((nd, batch, chans), jnp.float32),
            dma, dma,
        ] + gathers + gathers + [dma, dma, dma((2,)), dma((2,)), dma, dma]
        + [dma((nv - 1,))] * 4 + [dma((nd,))] * 4,
        compiler_params=pltpu.CompilerParams(
            collective_id=2, has_side_effects=True, vmem_limit_bytes=56 * 1024 * 1024
        ),
        cost_estimate=pl.CostEstimate(flops=0, bytes_accessed=int(90 * 3.0e6), transcendentals=0),
        name="front",
    )(resid, gain, in_x, in_z, conv_w, conv_b, low_w, dt_gain, proj, bias, rate)


def back_kernel(
    nv, nd, steps, relay_at, gated_ref, w_ref, resid_ref, gain_ref, head_ref, ids_ref, mask_ref,
    hidden_ref, logp_ref, sum_ref,
    weight, own, near, send_up, recv_up, send_down, recv_down, hid, fin, full, logits, ids, stats, heard,
    part, parts, w_sem, near_sem, up_s, up_r, down_s, down_r, gup_s, gup_r, gdown_s, gdown_r,
    fin_s, fin_r, ids_s, ids_r, head_l, head_s, head_r, pass_s, pass_r, stat_s, stat_r, sum_s, sum_r,
):
    me = lax.axis_index("vocab")
    dev = lax.axis_index("dp")
    chip, core = dev // 2, lax.rem(dev, 2)
    mate = {"dp": chip * 2 + 1 - core}
    above, below = {"vocab": lax.rem(me + 1, nv)}, {"vocab": lax.rem(me + nv - 1, nv)}
    rows, chans = gated_ref.shape
    width = w_ref.shape[1]
    share = width // nv
    entries, feats = head_ref.shape
    half = entries // 2
    size = rows // steps

    def block(index, length):
        return pl.ds(pl.multiple_of(index * length, length), length)

    weight_copies = []
    for s in range(nv):
        index = jnp.where(me * 2 < nv, nv - 1 - s, s)
        copy = pltpu.make_async_copy(
            w_ref.at[:, block(index, share)], weight.at[:, block(index, share)], w_sem.at[s]
        )
        copy.start()
        weight_copies.append((index, copy))
    near_copy = pltpu.make_async_copy(resid_ref.at[:, block(me, share)], near, near_sem)
    near_copy.start()
    greet_back(nv, nd)

    head_waits, head_sends, passes = gather_halves(
        nd, lambda c: head_ref.at[block(c, half)], lambda d: full.at[:, block(d, feats)], half,
        head_l, head_s, head_r, pass_s, pass_r,
    )
    mine = ids.at[core]
    ids[core] = ids_ref[...]
    ids_copy = remote(ids_ref, mine, ids_s, ids_r, mate)
    ids_copy.start()

    def up(i, j):
        return remote(send_up.at[i, j - 1], recv_up.at[i, j - 1], up_s.at[i, j - 1], up_r.at[i, j - 1], above)

    def down(i, j):
        return remote(send_down.at[i, j], recv_down.at[i, j], down_s.at[i, j], down_r.at[i, j], below)

    def spread_up(i, s):
        at = hid.at[block(i, size), block(s, share)]
        return remote(at, at, gup_s.at[i, s], gup_r.at[i, s], above)

    def spread_down(i, s):
        at = hid.at[block(i, size), block(s, share)]
        return remote(at, at, gdown_s.at[i, s - 1], gdown_r.at[i, s - 1], below)

    def fin_copy(i):
        at = fin.at[core, block(i, size)]
        return remote(at, at, fin_s.at[i], fin_r.at[i], mate)

    tile = min(512, share)
    for index, copy in weight_copies:
        copy.wait()

        @pl.loop(0, share // tile)
        def _(k):
            at = pl.ds(pl.multiple_of(index * share + k * tile, tile), tile)
            own[:, at] = jnp.dot(gated_ref[...], weight[:, at], preferred_element_type=jnp.float32)

        @pl.when((me == 0) & (index > 0))
        def _():
            @pl.loop(0, steps)
            def _(i):
                send_up[i, index - 1] = own[block(i, size), block(index, share)].astype(jnp.bfloat16)
                up(i, index).start()

        @pl.when((me == nv - 1) & (index < nv - 1))
        def _():
            @pl.loop(0, steps)
            def _(i):
                send_down[i, index] = own[block(i, size), block(index, share)].astype(jnp.bfloat16)
                down(i, index).start()

    near_copy.wait()

    def combine_up(i):
        for j in range(nv - 1, 0, -1):
            @pl.when((me > 0) & (me < j))
            def _():
                up(i, j).wait_recv()
                send_up[i, j - 1] = (
                    own[block(i, size), pl.ds(j * share, share)] + recv_up[i, j - 1].astype(jnp.float32)
                ).astype(jnp.bfloat16)
                up(i, j).start()

    def combine_down(i):
        for j in range(nv - 1):
            @pl.when((me < nv - 1) & (me > j))
            def _():
                down(i, j).wait_recv()
                send_down[i, j] = (
                    own[block(i, size), pl.ds(j * share, share)] + recv_down[i, j].astype(jnp.float32)
                ).astype(jnp.bfloat16)
                down(i, j).start()

    def finish(i):
        at = block(i, size)
        own[at, block(me, share)] = own[at, block(me, share)] + near[at, :].astype(jnp.float32)

        @pl.when(me > 0)
        def _():
            up(i, me).wait_recv()
            own[at, block(me, share)] = own[at, block(me, share)] + recv_up[i, me - 1].astype(jnp.float32)

        @pl.when(me < nv - 1)
        def _():
            down(i, me).wait_recv()
            own[at, block(me, share)] = own[at, block(me, share)] + recv_down[i, me].astype(jnp.float32)

        value = own[at, block(me, share)].astype(jnp.bfloat16)
        hidden_ref[at, :] = value
        hid[at, block(me, share)] = value

        @pl.when(me < nv - 1)
        def _():
            spread_up(i, me).start()

        @pl.when(me > 0)
        def _():
            spread_down(i, me).start()

    def forward(i, hops):
        low, high = me - hops, me + hops

        @pl.when(low >= 0)
        def _():
            spread_up(i, low).wait_recv()

            @pl.when(me < nv - 1)
            def _():
                spread_up(i, low).start()

        @pl.when(high < nv)
        def _():
            spread_down(i, high).wait_recv()

            @pl.when(me > 0)
            def _():
                spread_down(i, high).start()

    def normalize(i):
        at = block(i, size)
        wide = hid[at, :].astype(jnp.float32)
        scale = lax.rsqrt(jnp.mean(wide * wide, axis=-1, keepdims=True) + 1e-05)
        fin[core, at] = (wide * scale * gain_ref[...]).astype(jnp.bfloat16)
        fin_copy(i).start()

    late = jnp.where(me * 2 >= nv, 1, 0)

    def walk(first, last):
        @pl.loop(first, last)
        def _(t):
            def at(i, step):
                @pl.when((i >= 0) & (i < steps))
                def _():
                    step(i)

            at(t - late, combine_up)
            at(t - 1 + late, combine_down)
            at(t - 2, finish)
            for hops in range(1, nv):
                at(t - 2 - hops, functools.partial(forward, hops=hops))
            at(t - 1 - nv, normalize)

    walk(0, relay_at)
    passes()
    walk(relay_at, steps + nv + 1)

    @pl.loop(0, steps)
    def _(i):
        remote(
            fin.at[core, block(i, size)], fin.at[1 - core, block(i, size)], fin_s.at[i], fin_r.at[i], mate
        ).wait_recv()
    ids_copy.wait()
    head_waits()

    vt = min(256, half)
    for s in range(2):
        @pl.loop(0, half // vt)
        def _(k):
            logits[block(k, vt), s * rows : (s + 1) * rows] = lax.dot_general(
                full[block(k, vt), :], fin[s], (((1,), (1,)), ((), ())), preferred_element_type=jnp.float32
            )

        def highest(k, top):
            return jnp.maximum(
                top, jnp.max(logits[block(k, vt), s * rows : (s + 1) * rows], axis=0, keepdims=True)
            )

        top = lax.fori_loop(0, half // vt, highest, jnp.full((1, rows), -jnp.inf, jnp.float32))
        wanted = ids[s, 0:1, :] - (me * entries + core * half)

        def gather(k, carry):
            total, picked = carry
            values = logits[block(k, vt), s * rows : (s + 1) * rows]
            entry = lax.broadcasted_iota(jnp.int32, values.shape, 0) + k * vt
            total = total + jnp.sum(jnp.exp(values - top), axis=0, keepdims=True)
            picked = picked + jnp.sum(jnp.where(entry == wanted, values, 0.0), axis=0, keepdims=True)
            return total, picked

        zero = jnp.zeros((1, rows), jnp.float32)
        total, picked = lax.fori_loop(0, half // vt, gather, (zero, zero))
        stats[s, 0:1, :] = top
        stats[s, 1:2, :] = total
        stats[s, 2:3, :] = picked
        stats[s, 3:8, :] = jnp.zeros((5, rows), jnp.float32)

    sends = []
    for shift in range(nv):
        for other in range(2):
            if shift == 0 and other == 0:
                continue
            owner = core if other == 0 else 1 - core
            copy = remote(
                stats.at[owner], heard.at[me, core], stat_s.at[shift, other], stat_r.at[me, core],
                {"vocab": lax.rem(me + shift, nv), "dp": chip * 2 + owner},
            )
            copy.start()
            sends.append(copy)
    heard[me, core] = stats[core]
    for z in range(nv):
        for c in range(2):
            @pl.when((z != me) | (c != core))
            def _():
                remote(stats.at[0], heard.at[z, c], stat_s.at[0, 1], stat_r.at[z, c], mate).wait_recv()
    everyone = [heard[z, c] for z in range(nv) for c in range(2)]
    top = everyone[0][0:1]
    for one in everyone[1:]:
        top = jnp.maximum(top, one[0:1])
    total = jnp.zeros_like(top)
    picked = jnp.zeros_like(top)
    for one in everyone:
        total = total + one[1:2] * jnp.exp(one[0:1] - top)
        picked = picked + one[2:3]
    logp = picked - (top + jnp.log(total))
    logp_ref[...] = logp
    masked = jnp.sum(jnp.where(mask_ref[...] > 0.0, logp, 0.0), axis=-1, keepdims=True)
    part[...] = jnp.broadcast_to(masked, part.shape)
    for shift in range(1, nd):
        copy = remote(
            part, parts.at[dev], sum_s.at[shift - 1], sum_r.at[dev], {"dp": lax.rem(dev + shift, nd)}
        )
        copy.start()
        sends.append(copy)
    parts[dev] = part[...]
    for d in range(nd):
        @pl.when(d != dev)
        def _():
            remote(part, parts.at[d], sum_s.at[0], sum_r.at[d], mate).wait_recv()
    grand = parts[0]
    for d in range(1, nd):
        grand = grand + parts[d]
    sum_ref[...] = grand

    for copy in sends:
        copy.wait_send()
    head_sends()

    @pl.loop(0, steps)
    def _(i):
        fin_copy(i).wait_send()
        for j in range(1, nv):
            @pl.when(me < j)
            def _():
                up(i, j).wait_send()
        for j in range(nv - 1):
            @pl.when(me > j)
            def _():
                down(i, j).wait_send()
        for s in range(nv - 1):
            @pl.when((me >= s) & (me < nv - 1))
            def _():
                spread_up(i, s).wait_send()
        for s in range(1, nv):
            @pl.when((me <= s) & (me > 0))
            def _():
                spread_down(i, s).wait_send()


def greet_back(nv, nd):
    barrier = pltpu.get_barrier_semaphore()
    me, dev = lax.axis_index("vocab"), lax.axis_index("dp")
    mate = dev // 2 * 2 + 1 - lax.rem(dev, 2)
    for shift in range(1, nd):
        pl.semaphore_signal(barrier, inc=1, device_id=peer("dp", shift), device_id_type=MESH)
    for shift in range(1, nv):
        z = lax.rem(me + shift, nv)
        pl.semaphore_signal(barrier, inc=1, device_id={"vocab": z}, device_id_type=MESH)
        pl.semaphore_signal(barrier, inc=1, device_id={"vocab": z, "dp": mate}, device_id_type=MESH)
    pl.semaphore_wait(barrier, nd - 1 + 2 * (nv - 1))


def gather_halves(nd, source, target, length, local, send, recv, pass_s, pass_r):
    dev = lax.axis_index("dp")
    chip, core = dev // 2, lax.rem(dev, 2)
    keep = pltpu.make_async_copy(source(core), target(dev), local)
    keep.start()
    copies = [remote(source(1 - core), target(dev), send.at[0, 0], recv.at[0, core], {"dp": chip * 2 + 1 - core})]
    copies[0].start()
    waits = [remote(source(0), target(chip * 2 + 1 - core), send.at[0, 0], recv.at[0, 1 - core], {"dp": dev})]
    if nd != 8:
        for shift in range(1, nd // 2):
            there = lax.rem(chip + shift, nd // 2)
            back = lax.rem(chip + nd // 2 - shift, nd // 2)
            for c in range(2):
                copy = remote(
                    source(c), target(dev), send.at[shift, c], recv.at[shift, core], {"dp": there * 2 + c}
                )
                copy.start()
                copies.append(copy)
                waits.append(
                    remote(source(c), target(back * 2 + c), send.at[shift, c], recv.at[shift, c], {"dp": dev})
                )
        passes = lambda: None
    else:
        piece = length // 2
        sides = (chip + 1 - 2 * lax.rem(chip, 2), lax.rem(chip + 2, 4))

        def at(ref, p):
            return ref.at[pl.ds(p * piece, piece)]

        first = []
        for turn in range(2):
            for side in range(2):
                p = side if turn == 0 else 1 - side
                for c in range(2):
                    k = 1 + side * 2 + p
                    copy = remote(
                        at(source(c), p), at(target(dev), p), send.at[k, c], recv.at[k, core],
                        {"dp": sides[side] * 2 + c},
                    )
                    copy.start()
                    copies.append(copy)
                    came = at(target(sides[side] * 2 + c), p)
                    wait = remote(came, came, send.at[k, c], recv.at[k, c], {"dp": dev})
                    if turn == 0:
                        first.append((side, p, c, wait, came))
                    else:
                        waits.append(wait)

        far = 3 - chip
        for side in range(2):
            for c in range(2):
                came = at(target(far * 2 + c), 1 - side)
                waits.append(
                    remote(came, came, pass_s.at[side, c], pass_r.at[1 - side, c], {"dp": dev})
                )

        def passes():
            for side, p, c, wait, came in first:
                wait.wait_recv()
                copy = remote(
                    came, came, pass_s.at[side, c], pass_r.at[p, c], {"dp": sides[1 - side] * 2 + core}
                )
                copy.start()
                copies.append(copy)

    def finish_waits():
        keep.wait()
        for wait in waits:
            wait.wait_recv()

    def finish_sends():
        for copy in copies:
            copy.wait_send()

    return finish_waits, finish_sends, passes


def back(gated, w, resid, gain, head, ids, mask, nv, nd, steps=4, relay_at=3):
    rows, chans = gated.shape
    width = w.shape[1]
    share = width // nv
    half = head.shape[0] // 2
    size = rows // steps
    dma = pltpu.SemaphoreType.DMA
    line = pltpu.VMEM((steps, nv - 1, size, share), jnp.bfloat16)
    lanes = 5 if nd == 8 else nd // 2
    anywhere = pl.BlockSpec(memory_space=pl.ANY)
    return pl.pallas_call(
        functools.partial(back_kernel, nv, nd, steps, relay_at),
        out_shape=(
            jax.ShapeDtypeStruct((rows, share), jnp.bfloat16),
            jax.ShapeDtypeStruct((1, rows), jnp.float32),
            jax.ShapeDtypeStruct((8, LANE), jnp.float32),
        ),
        in_specs=[VMEM, anywhere, anywhere, VMEM, anywhere, VMEM, VMEM],
        out_specs=(VMEM, VMEM, VMEM),
        scratch_shapes=[
            pltpu.VMEM((chans, width), jnp.bfloat16),
            pltpu.VMEM((rows, width), jnp.float32),
            pltpu.VMEM((rows, share), jnp.bfloat16),
            line, line, line, line,
            pltpu.VMEM((rows, width), jnp.bfloat16),
            pltpu.VMEM((2, rows, width), jnp.bfloat16),
            pltpu.VMEM((half, width), jnp.bfloat16),
            pltpu.VMEM((half, 2 * rows), jnp.float32),
            pltpu.VMEM((2, 8, rows), jnp.int32),
            pltpu.VMEM((2, 8, rows), jnp.float32),
            pltpu.VMEM((nv, 2, 8, rows), jnp.float32),
            pltpu.VMEM((8, LANE), jnp.float32),
            pltpu.VMEM((nd, 8, LANE), jnp.float32),
            dma((nv,)), dma,
        ] + [dma((steps, nv - 1))] * 8 + [
            dma((steps,)), dma((steps,)), dma, dma, dma, dma((lanes, 2)), dma((lanes, 2)),
            dma((2, 2)), dma((2, 2)), dma((nv, 2)), dma((nv, 2)), dma((nd,)), dma((nd,)),
        ],
        compiler_params=pltpu.CompilerParams(
            collective_id=3, has_side_effects=True, vmem_limit_bytes=60 * 1024 * 1024
        ),
        cost_estimate=pl.CostEstimate(flops=0, bytes_accessed=int(80 * 3.0e6), transcendentals=0),
        name="back",
    )(gated, w, resid, gain, head, ids, mask)


def body(
    resid, norm_gain, in_x, in_z, conv_w, conv_b, xdt_w, xbc_w, dt_gain, dt_proj, dt_bias,
    a_rate, out_w, final_gain, head_w, targets, lengths,
):
    nv, nd = lax.axis_size("vocab"), lax.axis_size("dp")
    batch, local_len, width = resid.shape
    channels = in_x.shape[1]
    nstate = a_rate.shape[1]
    rows = batch * local_len

    pad = -(2 * nstate) % 128
    low_w = jnp.concatenate([xdt_w, xbc_w, jnp.zeros((channels, pad), jnp.bfloat16)], axis=1)
    flat = resid.reshape(rows, width)
    gated = front(
        flat, norm_gain[None, :], in_x, in_z, conv_w, conv_b[None, :], low_w, dt_gain[None, :], dt_proj,
        dt_bias[None, :], a_rate.T, batch, nv, nd,
    )
    share = width // nv
    positions = lax.axis_index("dp") * local_len + jnp.arange(local_len, dtype=jnp.int32)
    mask = (positions[None, :] < lengths[:, None]).astype(jnp.float32).reshape(1, rows)
    ids = jnp.broadcast_to(targets.reshape(1, rows), (8, rows))
    hidden_share, logp, grand = back(gated, out_w, flat, final_gain[None, :], head_w, ids, mask, nv, nd)
    mean_logp = grand[0, 0] / jnp.sum(lengths.astype(jnp.float32))
    return (
        hidden_share.reshape(batch, local_len, share),
        logp.reshape(batch, local_len),
        mean_logp,
    )


def solution(mesh):
    in_specs = (
        P(None, "dp", None), P(), P("dp", "vocab"), P("dp", "vocab"), P(None, "vocab"), P("vocab"),
        P("vocab", None), P("vocab", None), P(), P(None, "vocab"), P("vocab"), P("vocab", None),
        P("vocab", None), P(), P("vocab", "dp"), P(None, "dp"), P(),
    )
    out_specs = (P(None, "dp", "vocab"), P(None, "dp"), P())
    return jax.shard_map(body, mesh=mesh, in_specs=in_specs, out_specs=out_specs, check_vma=False)
```

```python
import functools

import jax
import jax.numpy as jnp
from jax import lax
from jax.experimental import pallas as pl
from jax.experimental.pallas import tpu as pltpu
from jax.sharding import PartitionSpec as P

MESH = pl.DeviceIdType.MESH
VMEM = pl.BlockSpec(memory_space=pltpu.VMEM)
CHUNKS = 8
LANE = 128


def peer(axis, shift):
    size = lax.axis_size(axis)
    return {axis: lax.rem(lax.axis_index(axis) + shift, size)}


def greet(axes):
    barrier = pltpu.get_barrier_semaphore()
    count = 0
    for axis in axes:
        for shift in range(1, lax.axis_size(axis)):
            pl.semaphore_signal(barrier, inc=1, device_id=peer(axis, shift), device_id_type=MESH)
            count += 1
    pl.semaphore_wait(barrier, count)


def remote(src, dst, send_sem, recv_sem, device):
    return pltpu.make_async_remote_copy(
        src_ref=src, dst_ref=dst, send_sem=send_sem, recv_sem=recv_sem,
        device_id=device, device_id_type=MESH,
    )


def front_kernel(
    nv, nd, batch, ranks, nstate, resid_ref, gain_ref, in_x_ref, in_z_ref, conv_w_ref, conv_b_ref, xdt_ref, xbc_ref,
    dt_gain_ref, proj_ref, bias_ref, rate_ref, gated_ref,
    normed, full_x, full_z, made, whole, zwhole, edge, padded, act, part, low_recv, low_mine, low,
    step, drive, maps, result, decay, spread, state, sums, agg, tot, agg_in, tot_in,
    norm_s, norm_r, x_l, x_s, x_r, xp_s, xp_r, z_l, z_s, z_r, zp_s, zp_r,
    swap_s, swap_r, edge_s, edge_r, zswap_s, zswap_r, l1_s, l1_r, l2_s, l2_r, s1, r1, s2, r2,
):
    me = lax.axis_index("dp")
    chip, core = me // 2, lax.rem(me, 2)
    mate = {"dp": chip * 2 + 1 - core}
    vme = lax.axis_index("vocab")
    rows, width = resid_ref.shape
    feats, chans = in_x_ref.shape
    half = chans // 2
    length = rows // batch
    greet(("dp", "vocab"))

    def columns(c):
        return pl.ds(pl.multiple_of(c * half, half), half)

    def block(index, size):
        return pl.ds(pl.multiple_of(index * size, size), size)

    x_waits, x_sends, x_passes = gather_halves(
        nd, lambda c: in_x_ref.at[:, columns(c)], lambda d: full_x.at[block(d, feats)], feats,
        x_l, x_s, x_r, xp_s, xp_r,
    )
    piece = min(32, rows)

    @pl.loop(0, rows // piece)
    def _(i):
        at = block(i, piece)
        wide = resid_ref[at, :].astype(jnp.float32)
        scale = lax.rsqrt(jnp.mean(wide * wide, axis=-1, keepdims=True) + 1e-05)
        normed[core, at] = (wide * scale * gain_ref[...]).astype(jnp.bfloat16)

    norm_copy = remote(normed.at[core], normed.at[core], norm_s, norm_r, mate)
    norm_copy.start()
    remote(normed.at[core], normed.at[1 - core], norm_s, norm_r, mate).wait_recv()
    x_passes()
    x_waits()
    tile = min(256, half)

    def project(full, r):
        @pl.loop(0, half // tile)
        def _(k):
            value = jnp.dot(normed[r], full[:, block(k, tile)], preferred_element_type=jnp.float32)
            made[r, :, :, block(k, tile)] = value.astype(jnp.bfloat16).reshape(batch, length, tile)

    def swap(send, recv):
        return remote(made.at[1 - core], whole.at[:, :, columns(core)], send, recv, mate)

    def swapped(send, recv):
        return remote(made.at[core], whole.at[:, :, columns(1 - core)], send, recv, mate)

    def zswap(send, recv):
        return remote(made.at[1 - core], zwhole.at[:, :, columns(core)], send, recv, mate)

    def zswapped(send, recv):
        return remote(made.at[core], zwhole.at[:, :, columns(1 - core)], send, recv, mate)

    project(full_x, 1 - core)
    swap(swap_s, swap_r).start()
    project(full_x, core)
    whole[:, :, columns(core)] = made[core]
    last = length - 16

    def tail_of(r):
        return made.at[r, :, pl.ds(last, 16), :]

    def tail_at(c):
        return edge.at[:, :, columns(c)]

    onward = {"dp": lax.rem(chip + 1, nd // 2) * 2}
    across = {"dp": chip * 2 + 1}

    @pl.when(core == 0)
    def _():
        remote(tail_of(0), tail_at(core), edge_s.at[0], edge_r.at[core], across).start()

    @pl.when(core == 1)
    def _():
        edge[:, :, columns(core)] = made[0, :, pl.ds(last, 16), :]

    @pl.when(chip < nd // 2 - 1)
    def _():
        remote(tail_of(1), tail_at(core), edge_s.at[1], edge_r.at[core], onward).start()

    z_waits, z_sends, z_passes = gather_halves(
        nd, lambda c: in_z_ref.at[:, columns(c)], lambda d: full_z.at[block(d, feats)], feats,
        z_l, z_s, z_r, zp_s, zp_r,
    )

    @pl.when(me == 0)
    def _():
        edge[...] = jnp.zeros_like(edge)

    swapped(swap_s, swap_r).wait_recv()
    swap(swap_s, swap_r).wait_send()

    @pl.when(core == 1)
    def _():
        remote(tail_of(0), tail_at(0), edge_s.at[0], edge_r.at[0], mate).wait_recv()

    @pl.when((core == 0) & (chip > 0))
    def _():
        for c in range(2):
            remote(tail_of(1), tail_at(c), edge_s.at[1], edge_r.at[c], mate).wait_recv()

    taps = conv_w_ref.shape[0]
    lane = min(256, chans)

    @pl.loop(0, chans // lane)
    def _(k):
        cols = block(k, lane)
        for b in range(batch):
            padded[0:8, :] = edge[b, 8:16, cols].astype(jnp.float32)
            padded[8:, :] = whole[b, :, cols].astype(jnp.float32)
            total = jnp.zeros((length, lane), jnp.float32) + conv_b_ref[:, cols]
            for tap in range(taps):
                first = 8 - (taps - 1) + tap
                total = total + conv_w_ref[tap : tap + 1, cols] * padded[first : first + length, :]
            act[b * length : (b + 1) * length, cols] = total / (1.0 + jnp.exp(-total))

    act_low = act[...].astype(jnp.bfloat16)
    part[:, ranks:] = jnp.zeros((rows, part.shape[1] - ranks), jnp.bfloat16)
    part[:, :ranks] = jnp.dot(act_low, xdt_ref[...], preferred_element_type=jnp.float32).astype(jnp.bfloat16)
    part[:, ranks : ranks + 2 * nstate] = lax.dot_general(
        act_low, xbc_ref[...], (((1,), (1,)), ((), ())), preferred_element_type=jnp.float32
    ).astype(jnp.bfloat16)

    share = rows // nv
    copies = []
    for shift in range(1, nv):
        target = lax.rem(vme + shift, nv)
        copy = remote(
            part.at[block(target, share)], low_recv.at[shift - 1],
            l1_s.at[shift - 1], l1_r.at[shift - 1], peer("vocab", shift),
        )
        copy.start()
        copies.append(copy)
    own = block(vme, share)
    total = part[own, :].astype(jnp.float32)
    for shift in range(1, nv):
        copies[shift - 1].wait()
        total = total + low_recv[shift - 1].astype(jnp.float32)
    dt = total[:, :ranks]
    scale = lax.rsqrt(jnp.mean(dt * dt, axis=-1, keepdims=True) + 1e-06)
    low_mine[:, :ranks] = (dt * scale * dt_gain_ref[...]).astype(jnp.bfloat16)
    low_mine[:, ranks:] = total[:, ranks:].astype(jnp.bfloat16)
    copies = []
    for shift in range(1, nv):
        copy = remote(low_mine, low.at[own], l2_s.at[shift - 1], l2_r.at[shift - 1], peer("vocab", shift))
        copy.start()
        copies.append(copy)
    low[own, :] = low_mine[...]
    for copy in copies:
        copy.wait()

    lanes = chans // LANE
    span = length // CHUNKS
    low_dt = low[:, :ranks]
    maps[...] = low[:, ranks:].astype(jnp.float32)
    wide = 2 if lanes % 2 == 0 else 1
    size = wide * LANE

    @pl.loop(0, lanes // wide)
    def _(g):
        cols = pl.ds(pl.multiple_of(g * size, size), size)
        raw = jnp.dot(
            low_dt, proj_ref[:, cols], preferred_element_type=jnp.float32
        ) + bias_ref[:, cols]
        value = jnp.maximum(raw, 0.0) + jnp.log1p(jnp.exp(-jnp.abs(raw)))
        pushed = value * act[:, cols]
        for w in range(wide):
            k = g * wide + w
            step[k] = value[:, w * LANE : (w + 1) * LANE]
            drive[k] = pushed[:, w * LANE : (w + 1) * LANE]

    @pl.loop(0, batch * span)
    def _(q):
        b = q // span
        both = maps[pl.ds(b * length + q - b * span, CHUNKS, stride=span), :]
        for n in range(2 * nstate):
            spread[n, block(q, CHUNKS), :] = jnp.broadcast_to(both[:, n : n + 1], (CHUNKS, LANE))

    def local_scan(group):
        @pl.loop(0, lanes // group)
        def _(g):
            for b in range(batch):
                rates = [
                    [
                        rate_ref[pl.ds(n, 1), pl.ds(pl.multiple_of((g * group + w) * LANE, LANE), LANE)]
                        for n in range(nstate)
                    ]
                    for w in range(group)
                ]

                def one(t, carry):
                    at = pl.ds(b * length + t, CHUNKS, stride=span)
                    held, extra = carry
                    held, extra = list(held), list(extra)
                    now = [step[g * group + w, at, :] for w in range(group)]
                    push = [drive[g * group + w, at, :] for w in range(group)]
                    for n in range(nstate):
                        into = spread[n, block(b * span + t, CHUNKS), :]
                        for w in range(group):
                            i = w * nstate + n
                            factor = jnp.exp(-now[w] * rates[w][n])
                            decay[b * span + t, g * group + w, pl.ds(n * CHUNKS, CHUNKS), :] = factor
                            held[i] = factor * held[i] + push[w] * into
                    for w in range(group):
                        extra[w] = extra[w] + now[w]
                    return tuple(held), tuple(extra)

                zero = jnp.zeros((CHUNKS, LANE), jnp.float32)
                held, extra = lax.fori_loop(0, span, one, ((zero,) * (group * nstate), (zero,) * group))
                for w in range(group):
                    for n in range(nstate):
                        state[b, g * group + w, pl.ds(n * CHUNKS, CHUNKS), :] = held[w * nstate + n]
                    sums[b, g * group + w] = extra[w]

    def final_scan(group):
        @pl.loop(0, lanes // group)
        def _(g):
            for b in range(batch):
                def one(t, carry):
                    at = pl.ds(b * length + t, CHUNKS, stride=span)
                    held = list(carry)
                    push = [drive[g * group + w, at, :] for w in range(group)]
                    acc = [None] * group
                    for n in range(nstate):
                        into = spread[n, block(b * span + t, CHUNKS), :]
                        outof = spread[nstate + n, block(b * span + t, CHUNKS), :]
                        for w in range(group):
                            i = w * nstate + n
                            factor = decay[b * span + t, g * group + w, pl.ds(n * CHUNKS, CHUNKS), :]
                            held[i] = factor * held[i] + push[w] * into
                            term = held[i] * outof
                            acc[w] = term if acc[w] is None else acc[w] + term
                    for w in range(group):
                        result[g * group + w, at, :] = acc[w]
                    return tuple(held)

                lax.fori_loop(
                    0, span, one,
                    tuple(
                        state[b, g * group + w, pl.ds(n * CHUNKS, CHUNKS), :]
                        for w in range(group) for n in range(nstate)
                    ),
                )

    local_scan(2 if lanes % 2 == 0 else 1)

    @pl.loop(0, lanes)
    def _(k):
        cols = pl.ds(pl.multiple_of(k * LANE, LANE), LANE)
        rate = rate_ref[:, cols]
        for b in range(batch):
            carry = jnp.zeros((nstate, LANE), jnp.float32)
            for c in range(CHUNKS):
                part = state[b, k, pl.ds(c, nstate, stride=CHUNKS), :]
                carry = jnp.exp(-sums[b, k, pl.ds(c, 1), :] * rate) * carry + part
            agg[pl.ds(b * nstate, nstate), cols] = carry.astype(jnp.bfloat16)
            tot[pl.ds(b, 1), cols] = jnp.sum(sums[b, k], axis=0, keepdims=True)

    def pair(source, target):
        device = {"dp": target}
        return (
            remote(agg, agg_in.at[source], s1.at[target], r1.at[source], device),
            remote(tot, tot_in.at[source], s2.at[target], r2.at[source], device),
        )

    for other in range(nd):
        @pl.when(other > me)
        def _():
            for copy in pair(me, other):
                copy.start()

    for other in range(nd):
        @pl.when(other < me)
        def _():
            for copy in pair(other, me):
                copy.wait_recv()

    @pl.loop(0, lanes)
    def _(k):
        cols = pl.ds(pl.multiple_of(k * LANE, LANE), LANE)
        rate = rate_ref[:, cols]
        for b in range(batch):
            def earlier(d, carry):
                decay = jnp.exp(-tot_in[d, pl.ds(b, 1), cols] * rate)
                return decay * carry + agg_in[d, pl.ds(b * nstate, nstate), cols].astype(
                    jnp.float32
                )

            carry = lax.fori_loop(0, me, earlier, jnp.zeros((nstate, LANE), jnp.float32))
            for c in range(CHUNKS):
                at = pl.ds(c, nstate, stride=CHUNKS)
                part = state[b, k, at, :]
                state[b, k, at, :] = carry
                carry = jnp.exp(-sums[b, k, pl.ds(c, 1), :] * rate) * carry + part

    z_passes()
    final_scan(2 if lanes % 2 == 0 else 1)

    @pl.when(core == 0)
    def _():
        remote(tail_of(0), tail_at(core), edge_s.at[0], edge_r.at[core], across).wait_send()

    @pl.when(chip < nd // 2 - 1)
    def _():
        remote(tail_of(1), tail_at(core), edge_s.at[1], edge_r.at[core], onward).wait_send()

    z_waits()
    project(full_z, 1 - core)
    zswap(zswap_s, zswap_r).start()
    project(full_z, core)
    zwhole[:, :, columns(core)] = made[core]
    zswapped(zswap_s, zswap_r).wait_recv()

    @pl.loop(0, lanes)
    def _(k):
        cols = block(k, LANE)
        for b in range(batch):
            gate = zwhole[b, :, cols].astype(jnp.float32)
            at = pl.ds(b * length, length)
            gated_ref[at, cols] = (result[k, at] * (gate / (1.0 + jnp.exp(-gate)))).astype(jnp.bfloat16)

    for other in range(nd):
        @pl.when(other > me)
        def _():
            for copy in pair(me, other):
                copy.wait_send()
    norm_copy.wait_send()
    zswap(zswap_s, zswap_r).wait_send()
    x_sends()
    z_sends()


def front(resid, gain, in_x, in_z, conv_w, conv_b, xdt, xbc, dt_gain, proj, bias, rate, batch, nv, nd):
    rows, width = resid.shape
    chans = in_x.shape[1]
    half = chans // 2
    ranks = proj.shape[0]
    nstate = rate.shape[0]
    lanes = chans // LANE
    length = rows // batch
    cols = ranks + 2 * nstate + -(ranks + 2 * nstate) % LANE
    dma = pltpu.SemaphoreType.DMA
    big = pltpu.VMEM((lanes, rows, LANE), jnp.float32)
    slots = 5 if nd == 8 else nd // 2
    gathers = [dma, dma((slots, 2)), dma((slots, 2)), dma((2, 2)), dma((2, 2))]
    anywhere = pl.BlockSpec(memory_space=pl.ANY)
    return pl.pallas_call(
        functools.partial(front_kernel, nv, nd, batch, ranks, nstate),
        out_shape=jax.ShapeDtypeStruct((rows, chans), jnp.bfloat16),
        in_specs=[VMEM, VMEM, anywhere, anywhere] + [VMEM] * 8,
        out_specs=VMEM,
        scratch_shapes=[
            pltpu.VMEM((2, rows, width), jnp.bfloat16),
            pltpu.VMEM((width, half), jnp.bfloat16),
            pltpu.VMEM((width, half), jnp.bfloat16),
            pltpu.VMEM((2, batch, length, half), jnp.bfloat16),
            pltpu.VMEM((batch, length, chans), jnp.bfloat16),
            pltpu.VMEM((batch, length, chans), jnp.bfloat16),
            pltpu.VMEM((batch, 16, chans), jnp.bfloat16),
            pltpu.VMEM((length + 8, min(256, chans)), jnp.float32),
            pltpu.VMEM((rows, chans), jnp.float32),
            pltpu.VMEM((rows, cols), jnp.bfloat16),
            pltpu.VMEM((nv - 1, rows // nv, cols), jnp.bfloat16),
            pltpu.VMEM((rows // nv, cols), jnp.bfloat16),
            pltpu.VMEM((rows, cols), jnp.bfloat16),
            big, big,
            pltpu.VMEM((rows, cols - ranks), jnp.float32),
            big,
            pltpu.VMEM((rows // CHUNKS, lanes, nstate * CHUNKS, LANE), jnp.float32),
            pltpu.VMEM((2 * nstate, rows, LANE), jnp.float32),
            pltpu.VMEM((batch, lanes, nstate * CHUNKS, LANE), jnp.float32),
            pltpu.VMEM((batch, lanes, CHUNKS, LANE), jnp.float32),
            pltpu.VMEM((batch * nstate, chans), jnp.bfloat16),
            pltpu.VMEM((batch, chans), jnp.float32),
            pltpu.VMEM((nd, batch * nstate, chans), jnp.bfloat16),
            pltpu.VMEM((nd, batch, chans), jnp.float32),
            dma, dma,
        ] + gathers + gathers + [dma, dma, dma((2,)), dma((2,)), dma, dma]
        + [dma((nv - 1,))] * 4 + [dma((nd,))] * 4,
        compiler_params=pltpu.CompilerParams(
            collective_id=2, has_side_effects=True, vmem_limit_bytes=56 * 1024 * 1024
        ),
        cost_estimate=pl.CostEstimate(flops=0, bytes_accessed=int(90 * 3.0e6), transcendentals=0),
        name="front",
    )(resid, gain, in_x, in_z, conv_w, conv_b, xdt, xbc, dt_gain, proj, bias, rate)


def back_kernel(
    nv, nd, steps, relay_at, gated_ref, w_ref, resid_ref, gain_ref, head_ref, ids_ref, lengths_ref,
    hidden_ref, logp_ref, sum_ref,
    weight, own, near, send_up, recv_up, send_down, recv_down, hid, fin, full, logits, ids, stats, heard,
    part, parts, w_sem, near_sem, up_s, up_r, down_s, down_r, gup_s, gup_r, gdown_s, gdown_r,
    fin_s, fin_r, ids_s, ids_r, head_l, head_s, head_r, pass_s, pass_r, stat_s, stat_r, sum_s, sum_r,
):
    me = lax.axis_index("vocab")
    dev = lax.axis_index("dp")
    chip, core = dev // 2, lax.rem(dev, 2)
    mate = {"dp": chip * 2 + 1 - core}
    above, below = {"vocab": lax.rem(me + 1, nv)}, {"vocab": lax.rem(me + nv - 1, nv)}
    rows, chans = gated_ref.shape
    batch, length = ids_ref.shape
    width = w_ref.shape[1]
    share = width // nv
    entries, feats = head_ref.shape
    half = entries // 2
    size = rows // steps

    def block(index, length):
        return pl.ds(pl.multiple_of(index * length, length), length)

    weight_copies = []
    for s in range(nv):
        index = jnp.where(me * 2 < nv, nv - 1 - s, s)
        copy = pltpu.make_async_copy(
            w_ref.at[:, block(index, share)], weight.at[:, block(index, share)], w_sem.at[s]
        )
        copy.start()
        weight_copies.append((index, copy))
    near_copy = pltpu.make_async_copy(resid_ref.at[:, block(me, share)], near, near_sem)
    near_copy.start()
    greet_back(nv, nd)

    head_waits, head_sends, passes = gather_halves(
        nd, lambda c: head_ref.at[block(c, half)], lambda d: full.at[:, block(d, feats)], half,
        head_l, head_s, head_r, pass_s, pass_r,
    )
    mine = ids.at[core]
    ids[core] = ids_ref[...]
    ids_copy = remote(ids_ref, mine, ids_s, ids_r, mate)
    ids_copy.start()

    def up(i, j):
        return remote(send_up.at[i, j - 1], recv_up.at[i, j - 1], up_s.at[i, j - 1], up_r.at[i, j - 1], above)

    def down(i, j):
        return remote(send_down.at[i, j], recv_down.at[i, j], down_s.at[i, j], down_r.at[i, j], below)

    def spread_up(i, s):
        at = hid.at[block(i, size), block(s, share)]
        return remote(at, at, gup_s.at[i, s], gup_r.at[i, s], above)

    def spread_down(i, s):
        at = hid.at[block(i, size), block(s, share)]
        return remote(at, at, gdown_s.at[i, s - 1], gdown_r.at[i, s - 1], below)

    def fin_copy(i):
        at = fin.at[core, block(i, size)]
        return remote(at, at, fin_s.at[i], fin_r.at[i], mate)

    tile = min(512, share)
    for index, copy in weight_copies:
        copy.wait()

        @pl.loop(0, share // tile)
        def _(k):
            at = pl.ds(pl.multiple_of(index * share + k * tile, tile), tile)
            own[:, at] = jnp.dot(gated_ref[...], weight[:, at], preferred_element_type=jnp.float32)

        @pl.when((me == 0) & (index > 0))
        def _():
            @pl.loop(0, steps)
            def _(i):
                send_up[i, index - 1] = own[block(i, size), block(index, share)].astype(jnp.bfloat16)
                up(i, index).start()

        @pl.when((me == nv - 1) & (index < nv - 1))
        def _():
            @pl.loop(0, steps)
            def _(i):
                send_down[i, index] = own[block(i, size), block(index, share)].astype(jnp.bfloat16)
                down(i, index).start()

    near_copy.wait()

    def combine_up(i):
        for j in range(nv - 1, 0, -1):
            @pl.when((me > 0) & (me < j))
            def _():
                up(i, j).wait_recv()
                send_up[i, j - 1] = (
                    own[block(i, size), pl.ds(j * share, share)] + recv_up[i, j - 1].astype(jnp.float32)
                ).astype(jnp.bfloat16)
                up(i, j).start()

    def combine_down(i):
        for j in range(nv - 1):
            @pl.when((me < nv - 1) & (me > j))
            def _():
                down(i, j).wait_recv()
                send_down[i, j] = (
                    own[block(i, size), pl.ds(j * share, share)] + recv_down[i, j].astype(jnp.float32)
                ).astype(jnp.bfloat16)
                down(i, j).start()

    def finish(i):
        at = block(i, size)
        own[at, block(me, share)] = own[at, block(me, share)] + near[at, :].astype(jnp.float32)

        @pl.when(me > 0)
        def _():
            up(i, me).wait_recv()
            own[at, block(me, share)] = own[at, block(me, share)] + recv_up[i, me - 1].astype(jnp.float32)

        @pl.when(me < nv - 1)
        def _():
            down(i, me).wait_recv()
            own[at, block(me, share)] = own[at, block(me, share)] + recv_down[i, me].astype(jnp.float32)

        value = own[at, block(me, share)].astype(jnp.bfloat16)
        hidden_ref[at, :] = value
        hid[at, block(me, share)] = value

        @pl.when(me < nv - 1)
        def _():
            spread_up(i, me).start()

        @pl.when(me > 0)
        def _():
            spread_down(i, me).start()

    def forward(i, hops):
        low, high = me - hops, me + hops

        @pl.when(low >= 0)
        def _():
            spread_up(i, low).wait_recv()

            @pl.when(me < nv - 1)
            def _():
                spread_up(i, low).start()

        @pl.when(high < nv)
        def _():
            spread_down(i, high).wait_recv()

            @pl.when(me > 0)
            def _():
                spread_down(i, high).start()

    def normalize(i):
        at = block(i, size)
        wide = hid[at, :].astype(jnp.float32)
        scale = lax.rsqrt(jnp.mean(wide * wide, axis=-1, keepdims=True) + 1e-05)
        fin[core, at] = (wide * scale * gain_ref[...]).astype(jnp.bfloat16)
        fin_copy(i).start()

    late = jnp.where(me * 2 >= nv, 1, 0)

    def walk(first, last):
        @pl.loop(first, last)
        def _(t):
            def at(i, step):
                @pl.when((i >= 0) & (i < steps))
                def _():
                    step(i)

            at(t - late, combine_up)
            at(t - 1 + late, combine_down)
            at(t - 2, finish)
            for hops in range(1, nv):
                at(t - 2 - hops, functools.partial(forward, hops=hops))
            at(t - 1 - nv, normalize)

    walk(0, relay_at)
    passes()
    walk(relay_at, steps + nv + 1)

    @pl.loop(0, steps)
    def _(i):
        remote(
            fin.at[core, block(i, size)], fin.at[1 - core, block(i, size)], fin_s.at[i], fin_r.at[i], mate
        ).wait_recv()
    ids_copy.wait()
    head_waits()

    vt = min(256, half)
    for s in range(2):
        @pl.loop(0, half // vt)
        def _(k):
            logits[block(k, vt), s * rows : (s + 1) * rows] = lax.dot_general(
                full[block(k, vt), :], fin[s], (((1,), (1,)), ((), ())), preferred_element_type=jnp.float32
            )

        def highest(k, top):
            return jnp.maximum(
                top, jnp.max(logits[block(k, vt), s * rows : (s + 1) * rows], axis=0, keepdims=True)
            )

        top = lax.fori_loop(0, half // vt, highest, jnp.full((1, rows), -jnp.inf, jnp.float32))
        wanted = jnp.concatenate([ids[s, b : b + 1, :] for b in range(batch)], axis=1) - (me * entries + core * half)

        def gather(k, carry):
            total, picked = carry
            values = logits[block(k, vt), s * rows : (s + 1) * rows]
            entry = lax.broadcasted_iota(jnp.int32, values.shape, 0) + k * vt
            total = total + jnp.sum(jnp.exp(values - top), axis=0, keepdims=True)
            picked = picked + jnp.sum(jnp.where(entry == wanted, values, 0.0), axis=0, keepdims=True)
            return total, picked

        zero = jnp.zeros((1, rows), jnp.float32)
        total, picked = lax.fori_loop(0, half // vt, gather, (zero, zero))
        stats[s, 0:1, :] = top
        stats[s, 1:2, :] = total
        stats[s, 2:3, :] = picked
        stats[s, 3:8, :] = jnp.zeros((5, rows), jnp.float32)

    sends = []
    for shift in range(nv):
        for other in range(2):
            if shift == 0 and other == 0:
                continue
            owner = core if other == 0 else 1 - core
            copy = remote(
                stats.at[owner], heard.at[me, core], stat_s.at[shift, other], stat_r.at[me, core],
                {"vocab": lax.rem(me + shift, nv), "dp": chip * 2 + owner},
            )
            copy.start()
            sends.append(copy)
    heard[me, core] = stats[core]
    for z in range(nv):
        for c in range(2):
            @pl.when((z != me) | (c != core))
            def _():
                remote(stats.at[0], heard.at[z, c], stat_s.at[0, 1], stat_r.at[z, c], mate).wait_recv()
    everyone = [heard[z, c] for z in range(nv) for c in range(2)]
    top = everyone[0][0:1]
    for one in everyone[1:]:
        top = jnp.maximum(top, one[0:1])
    total = jnp.zeros_like(top)
    picked = jnp.zeros_like(top)
    for one in everyone:
        total = total + one[1:2] * jnp.exp(one[0:1] - top)
        picked = picked + one[2:3]
    logp = picked - (top + jnp.log(total))
    place = lax.broadcasted_iota(jnp.int32, (1, length), 1) + dev * length
    masked = jnp.zeros((1, 1), jnp.float32)
    count = jnp.zeros((1, 1), jnp.float32)
    for b in range(batch):
        part_logp = logp[:, b * length : (b + 1) * length]
        logp_ref[b : b + 1, :] = part_logp
        masked = masked + jnp.sum(jnp.where(place < lengths_ref[b], part_logp, 0.0), axis=-1, keepdims=True)
        count = count + lengths_ref[b].astype(jnp.float32)
    part[...] = jnp.broadcast_to(masked, part.shape)
    for shift in range(1, nd):
        copy = remote(
            part, parts.at[dev], sum_s.at[shift - 1], sum_r.at[dev], {"dp": lax.rem(dev + shift, nd)}
        )
        copy.start()
        sends.append(copy)
    parts[dev] = part[...]
    for d in range(nd):
        @pl.when(d != dev)
        def _():
            remote(part, parts.at[d], sum_s.at[0], sum_r.at[d], mate).wait_recv()
    grand = parts[0]
    for d in range(1, nd):
        grand = grand + parts[d]
    sum_ref[...] = grand[0:1, 0:1] / count

    for copy in sends:
        copy.wait_send()
    head_sends()

    @pl.loop(0, steps)
    def _(i):
        fin_copy(i).wait_send()
        for j in range(1, nv):
            @pl.when(me < j)
            def _():
                up(i, j).wait_send()
        for j in range(nv - 1):
            @pl.when(me > j)
            def _():
                down(i, j).wait_send()
        for s in range(nv - 1):
            @pl.when((me >= s) & (me < nv - 1))
            def _():
                spread_up(i, s).wait_send()
        for s in range(1, nv):
            @pl.when((me <= s) & (me > 0))
            def _():
                spread_down(i, s).wait_send()


def greet_back(nv, nd):
    barrier = pltpu.get_barrier_semaphore()
    me, dev = lax.axis_index("vocab"), lax.axis_index("dp")
    mate = dev // 2 * 2 + 1 - lax.rem(dev, 2)
    for shift in range(1, nd):
        pl.semaphore_signal(barrier, inc=1, device_id=peer("dp", shift), device_id_type=MESH)
    for shift in range(1, nv):
        z = lax.rem(me + shift, nv)
        pl.semaphore_signal(barrier, inc=1, device_id={"vocab": z}, device_id_type=MESH)
        pl.semaphore_signal(barrier, inc=1, device_id={"vocab": z, "dp": mate}, device_id_type=MESH)
    pl.semaphore_wait(barrier, nd - 1 + 2 * (nv - 1))


def gather_halves(nd, source, target, length, local, send, recv, pass_s, pass_r):
    dev = lax.axis_index("dp")
    chip, core = dev // 2, lax.rem(dev, 2)
    keep = pltpu.make_async_copy(source(core), target(dev), local)
    keep.start()
    copies = [remote(source(1 - core), target(dev), send.at[0, 0], recv.at[0, core], {"dp": chip * 2 + 1 - core})]
    copies[0].start()
    waits = [remote(source(0), target(chip * 2 + 1 - core), send.at[0, 0], recv.at[0, 1 - core], {"dp": dev})]
    if nd != 8:
        for shift in range(1, nd // 2):
            there = lax.rem(chip + shift, nd // 2)
            back = lax.rem(chip + nd // 2 - shift, nd // 2)
            for c in range(2):
                copy = remote(
                    source(c), target(dev), send.at[shift, c], recv.at[shift, core], {"dp": there * 2 + c}
                )
                copy.start()
                copies.append(copy)
                waits.append(
                    remote(source(c), target(back * 2 + c), send.at[shift, c], recv.at[shift, c], {"dp": dev})
                )
        passes = lambda: None
    else:
        piece = length // 2
        sides = (chip + 1 - 2 * lax.rem(chip, 2), lax.rem(chip + 2, 4))

        def at(ref, p):
            return ref.at[pl.ds(p * piece, piece)]

        first = []
        for turn in range(2):
            for side in range(2):
                p = side if turn == 0 else 1 - side
                for c in range(2):
                    k = 1 + side * 2 + p
                    copy = remote(
                        at(source(c), p), at(target(dev), p), send.at[k, c], recv.at[k, core],
                        {"dp": sides[side] * 2 + c},
                    )
                    copy.start()
                    copies.append(copy)
                    came = at(target(sides[side] * 2 + c), p)
                    wait = remote(came, came, send.at[k, c], recv.at[k, c], {"dp": dev})
                    if turn == 0:
                        first.append((side, p, c, wait, came))
                    else:
                        waits.append(wait)

        far = 3 - chip
        for side in range(2):
            for c in range(2):
                came = at(target(far * 2 + c), 1 - side)
                waits.append(
                    remote(came, came, pass_s.at[side, c], pass_r.at[1 - side, c], {"dp": dev})
                )

        def passes():
            for side, p, c, wait, came in first:
                wait.wait_recv()
                copy = remote(
                    came, came, pass_s.at[side, c], pass_r.at[p, c], {"dp": sides[1 - side] * 2 + core}
                )
                copy.start()
                copies.append(copy)

    def finish_waits():
        keep.wait()
        for wait in waits:
            wait.wait_recv()

    def finish_sends():
        for copy in copies:
            copy.wait_send()

    return finish_waits, finish_sends, passes


def back(gated, w, resid, gain, head, ids, lengths, nv, nd, steps=4, relay_at=3):
    rows, chans = gated.shape
    width = w.shape[1]
    share = width // nv
    half = head.shape[0] // 2
    size = rows // steps
    dma = pltpu.SemaphoreType.DMA
    line = pltpu.VMEM((steps, nv - 1, size, share), jnp.bfloat16)
    lanes = 5 if nd == 8 else nd // 2
    anywhere = pl.BlockSpec(memory_space=pl.ANY)
    return pl.pallas_call(
        functools.partial(back_kernel, nv, nd, steps, relay_at),
        out_shape=(
            jax.ShapeDtypeStruct((rows, share), jnp.bfloat16),
            jax.ShapeDtypeStruct(ids.shape, jnp.float32),
            jax.ShapeDtypeStruct((1, 1), jnp.float32),
        ),
        in_specs=[VMEM, anywhere, anywhere, VMEM, anywhere, VMEM, pl.BlockSpec(memory_space=pltpu.SMEM)],
        out_specs=(VMEM, VMEM, VMEM),
        scratch_shapes=[
            pltpu.VMEM((chans, width), jnp.bfloat16),
            pltpu.VMEM((rows, width), jnp.float32),
            pltpu.VMEM((rows, share), jnp.bfloat16),
            line, line, line, line,
            pltpu.VMEM((rows, width), jnp.bfloat16),
            pltpu.VMEM((2, rows, width), jnp.bfloat16),
            pltpu.VMEM((half, width), jnp.bfloat16),
            pltpu.VMEM((half, 2 * rows), jnp.float32),
            pltpu.VMEM((2,) + ids.shape, jnp.int32),
            pltpu.VMEM((2, 8, rows), jnp.float32),
            pltpu.VMEM((nv, 2, 8, rows), jnp.float32),
            pltpu.VMEM((8, LANE), jnp.float32),
            pltpu.VMEM((nd, 8, LANE), jnp.float32),
            dma((nv,)), dma,
        ] + [dma((steps, nv - 1))] * 8 + [
            dma((steps,)), dma((steps,)), dma, dma, dma, dma((lanes, 2)), dma((lanes, 2)),
            dma((2, 2)), dma((2, 2)), dma((nv, 2)), dma((nv, 2)), dma((nd,)), dma((nd,)),
        ],
        compiler_params=pltpu.CompilerParams(
            collective_id=3, has_side_effects=True, vmem_limit_bytes=60 * 1024 * 1024
        ),
        cost_estimate=pl.CostEstimate(flops=0, bytes_accessed=int(80 * 3.0e6), transcendentals=0),
        name="back",
    )(gated, w, resid, gain, head, ids, lengths)


def body(
    resid, norm_gain, in_x, in_z, conv_w, conv_b, xdt_w, xbc_w, dt_gain, dt_proj, dt_bias,
    a_rate, out_w, final_gain, head_w, targets, lengths,
):
    nv, nd = lax.axis_size("vocab"), lax.axis_size("dp")
    batch, local_len, width = resid.shape
    channels = in_x.shape[1]
    rows = batch * local_len

    flat = resid.reshape(rows, width)
    gated = front(
        flat, norm_gain[None, :], in_x, in_z, conv_w, conv_b[None, :], xdt_w, xbc_w.T, dt_gain[None, :], dt_proj,
        dt_bias[None, :], a_rate.T, batch, nv, nd,
    )
    share = width // nv
    hidden_share, logp, mean_logp = back(
        gated, out_w, flat, final_gain[None, :], head_w, targets, lengths, nv, nd
    )
    return (
        hidden_share.reshape(batch, local_len, share),
        logp,
        mean_logp.reshape(()),
    )


def solution(mesh):
    in_specs = (
        P(None, "dp", None), P(), P("dp", "vocab"), P("dp", "vocab"), P(None, "vocab"), P("vocab"),
        P("vocab", None), P("vocab", None), P(), P(None, "vocab"), P("vocab"), P("vocab", None),
        P("vocab", None), P(), P("vocab", "dp"), P(None, "dp"), P(),
    )
    out_specs = (P(None, "dp", "vocab"), P(None, "dp"), P())
    return jax.shard_map(body, mesh=mesh, in_specs=in_specs, out_specs=out_specs, check_vma=False)
```

```python
import functools

import jax
import jax.numpy as jnp
from jax import lax
from jax.experimental import pallas as pl
from jax.experimental.pallas import tpu as pltpu
from jax.sharding import PartitionSpec as P

MESH = pl.DeviceIdType.MESH
VMEM = pl.BlockSpec(memory_space=pltpu.VMEM)
CHUNKS = 8
LANE = 128


def peer(axis, shift):
    size = lax.axis_size(axis)
    return {axis: lax.rem(lax.axis_index(axis) + shift, size)}


def greet(axes):
    barrier = pltpu.get_barrier_semaphore()
    count = 0
    for axis in axes:
        for shift in range(1, lax.axis_size(axis)):
            pl.semaphore_signal(barrier, inc=1, device_id=peer(axis, shift), device_id_type=MESH)
            count += 1
    pl.semaphore_wait(barrier, count)


def remote(src, dst, send_sem, recv_sem, device):
    return pltpu.make_async_remote_copy(
        src_ref=src, dst_ref=dst, send_sem=send_sem, recv_sem=recv_sem,
        device_id=device, device_id_type=MESH,
    )


def front_kernel(
    nv, nd, batch, ranks, nstate, resid_ref, gain_ref, in_x_ref, in_z_ref, conv_w_ref, conv_b_ref, xdt_ref, xbc_ref,
    dt_gain_ref, proj_ref, bias_ref, rate_ref, gated_ref,
    normed, full_x, full_z, made, whole, zwhole, edge, padded, act, part, low_recv, low_mine, low,
    step, drive, maps, result, decay, spread, state, sums, agg, tot, agg_in, tot_in,
    norm_s, norm_r, x_l, x_s, x_r, xp_s, xp_r, z_l, z_s, z_r, zp_s, zp_r,
    swap_s, swap_r, edge_s, edge_r, zswap_s, zswap_r, l1_s, l1_r, l2_s, l2_r, s1, r1, s2, r2,
):
    me = lax.axis_index("dp")
    chip, core = me // 2, lax.rem(me, 2)
    mate = {"dp": chip * 2 + 1 - core}
    vme = lax.axis_index("vocab")
    rows, width = resid_ref.shape
    feats, chans = in_x_ref.shape
    half = chans // 2
    length = rows // batch
    greet(("dp", "vocab"))

    def columns(c):
        return pl.ds(pl.multiple_of(c * half, half), half)

    def block(index, size):
        return pl.ds(pl.multiple_of(index * size, size), size)

    x_waits, x_sends, x_passes = gather_halves(
        nd, lambda c: in_x_ref.at[:, columns(c)], lambda d: full_x.at[block(d, feats)], feats,
        x_l, x_s, x_r, xp_s, xp_r,
    )
    piece = min(32, rows)

    @pl.loop(0, rows // piece)
    def _(i):
        at = block(i, piece)
        wide = resid_ref[at, :].astype(jnp.float32)
        scale = lax.rsqrt(jnp.mean(wide * wide, axis=-1, keepdims=True) + 1e-05)
        normed[core, at] = (wide * scale * gain_ref[...]).astype(jnp.bfloat16)

    norm_copy = remote(normed.at[core], normed.at[core], norm_s, norm_r, mate)
    norm_copy.start()
    remote(normed.at[core], normed.at[1 - core], norm_s, norm_r, mate).wait_recv()
    x_passes()
    x_waits()
    tile = min(256, half)

    def project(full, r):
        @pl.loop(0, half // tile)
        def _(k):
            value = jnp.dot(normed[r], full[:, block(k, tile)], preferred_element_type=jnp.float32)
            made[r, :, :, block(k, tile)] = value.astype(jnp.bfloat16).reshape(batch, length, tile)

    def swap(send, recv):
        return remote(made.at[1 - core], whole.at[:, :, columns(core)], send, recv, mate)

    def swapped(send, recv):
        return remote(made.at[core], whole.at[:, :, columns(1 - core)], send, recv, mate)

    def zswap(send, recv):
        return remote(made.at[1 - core], zwhole.at[:, :, columns(core)], send, recv, mate)

    def zswapped(send, recv):
        return remote(made.at[core], zwhole.at[:, :, columns(1 - core)], send, recv, mate)

    project(full_x, 1 - core)
    swap(swap_s, swap_r).start()
    project(full_x, core)
    whole[:, :, columns(core)] = made[core]
    last = length - 16

    def tail_of(r):
        return made.at[r, :, pl.ds(last, 16), :]

    def tail_at(c):
        return edge.at[:, :, columns(c)]

    onward = {"dp": lax.rem(chip + 1, nd // 2) * 2}
    across = {"dp": chip * 2 + 1}

    @pl.when(core == 0)
    def _():
        remote(tail_of(0), tail_at(core), edge_s.at[0], edge_r.at[core], across).start()

    @pl.when(core == 1)
    def _():
        edge[:, :, columns(core)] = made[0, :, pl.ds(last, 16), :]

    @pl.when(chip < nd // 2 - 1)
    def _():
        remote(tail_of(1), tail_at(core), edge_s.at[1], edge_r.at[core], onward).start()

    z_waits, z_sends, z_passes = gather_halves(
        nd, lambda c: in_z_ref.at[:, columns(c)], lambda d: full_z.at[block(d, feats)], feats,
        z_l, z_s, z_r, zp_s, zp_r,
    )

    @pl.when(me == 0)
    def _():
        edge[...] = jnp.zeros_like(edge)

    swapped(swap_s, swap_r).wait_recv()
    swap(swap_s, swap_r).wait_send()

    @pl.when(core == 1)
    def _():
        remote(tail_of(0), tail_at(0), edge_s.at[0], edge_r.at[0], mate).wait_recv()

    @pl.when((core == 0) & (chip > 0))
    def _():
        for c in range(2):
            remote(tail_of(1), tail_at(c), edge_s.at[1], edge_r.at[c], mate).wait_recv()

    taps = conv_w_ref.shape[0]
    lane = min(256, chans)

    @pl.loop(0, chans // lane)
    def _(k):
        cols = block(k, lane)
        for b in range(batch):
            padded[0:8, :] = edge[b, 8:16, cols].astype(jnp.float32)
            padded[8:, :] = whole[b, :, cols].astype(jnp.float32)
            total = jnp.zeros((length, lane), jnp.float32) + conv_b_ref[:, cols]
            for tap in range(taps):
                first = 8 - (taps - 1) + tap
                total = total + conv_w_ref[tap : tap + 1, cols] * padded[first : first + length, :]
            act[b * length : (b + 1) * length, cols] = total / (1.0 + jnp.exp(-total))

    act_low = act[...].astype(jnp.bfloat16)
    part[:, ranks:] = jnp.zeros((rows, part.shape[1] - ranks), jnp.bfloat16)
    part[:, :ranks] = jnp.dot(act_low, xdt_ref[...], preferred_element_type=jnp.float32).astype(jnp.bfloat16)
    part[:, ranks : ranks + 2 * nstate] = lax.dot_general(
        act_low, xbc_ref[...], (((1,), (1,)), ((), ())), preferred_element_type=jnp.float32
    ).astype(jnp.bfloat16)

    share = rows // nv
    copies = []
    for shift in range(1, nv):
        target = lax.rem(vme + shift, nv)
        copy = remote(
            part.at[block(target, share)], low_recv.at[shift - 1],
            l1_s.at[shift - 1], l1_r.at[shift - 1], peer("vocab", shift),
        )
        copy.start()
        copies.append(copy)
    own = block(vme, share)
    total = part[own, :].astype(jnp.float32)
    for shift in range(1, nv):
        copies[shift - 1].wait()
        total = total + low_recv[shift - 1].astype(jnp.float32)
    dt = total[:, :ranks]
    scale = lax.rsqrt(jnp.mean(dt * dt, axis=-1, keepdims=True) + 1e-06)
    low_mine[:, :ranks] = (dt * scale * dt_gain_ref[...]).astype(jnp.bfloat16)
    low_mine[:, ranks:] = total[:, ranks:].astype(jnp.bfloat16)
    copies = []
    for shift in range(1, nv):
        copy = remote(low_mine, low.at[own], l2_s.at[shift - 1], l2_r.at[shift - 1], peer("vocab", shift))
        copy.start()
        copies.append(copy)
    low[own, :] = low_mine[...]
    for copy in copies:
        copy.wait()

    lanes = chans // LANE
    span = length // CHUNKS
    low_dt = low[:, :ranks]
    maps[...] = low[:, ranks:].astype(jnp.float32)
    wide = 2 if lanes % 2 == 0 else 1
    size = wide * LANE

    @pl.loop(0, lanes // wide)
    def _(g):
        cols = pl.ds(pl.multiple_of(g * size, size), size)
        raw = jnp.dot(
            low_dt, proj_ref[:, cols], preferred_element_type=jnp.float32
        ) + bias_ref[:, cols]
        value = jnp.maximum(raw, 0.0) + jnp.log1p(jnp.exp(-jnp.abs(raw)))
        pushed = value * act[:, cols]
        for w in range(wide):
            k = g * wide + w
            step[k] = value[:, w * LANE : (w + 1) * LANE]
            drive[k] = pushed[:, w * LANE : (w + 1) * LANE]

    @pl.loop(0, batch * span)
    def _(q):
        b = q // span
        both = maps[pl.ds(b * length + q - b * span, CHUNKS, stride=span), :]
        for n in range(2 * nstate):
            spread[n, block(q, CHUNKS), :] = jnp.broadcast_to(both[:, n : n + 1], (CHUNKS, LANE))

    def local_scan(group):
        @pl.loop(0, lanes // group)
        def _(g):
            for b in range(batch):
                rates = [
                    [
                        rate_ref[pl.ds(n, 1), pl.ds(pl.multiple_of((g * group + w) * LANE, LANE), LANE)]
                        for n in range(nstate)
                    ]
                    for w in range(group)
                ]

                def one(t, carry):
                    at = pl.ds(b * length + t, CHUNKS, stride=span)
                    held, extra = carry
                    held, extra = list(held), list(extra)
                    now = [step[g * group + w, at, :] for w in range(group)]
                    push = [drive[g * group + w, at, :] for w in range(group)]
                    for n in range(nstate):
                        into = spread[n, block(b * span + t, CHUNKS), :]
                        for w in range(group):
                            i = w * nstate + n
                            factor = jnp.exp(-now[w] * rates[w][n])
                            decay[b * span + t, g * group + w, pl.ds(n * CHUNKS, CHUNKS), :] = factor
                            held[i] = factor * held[i] + push[w] * into
                    for w in range(group):
                        extra[w] = extra[w] + now[w]
                    return tuple(held), tuple(extra)

                zero = jnp.zeros((CHUNKS, LANE), jnp.float32)
                held, extra = lax.fori_loop(0, span, one, ((zero,) * (group * nstate), (zero,) * group))
                for w in range(group):
                    for n in range(nstate):
                        state[b, g * group + w, pl.ds(n * CHUNKS, CHUNKS), :] = held[w * nstate + n]
                    sums[b, g * group + w] = extra[w]

    def final_scan(group):
        @pl.loop(0, lanes // group)
        def _(g):
            for b in range(batch):
                def one(t, carry):
                    at = pl.ds(b * length + t, CHUNKS, stride=span)
                    held = list(carry)
                    push = [drive[g * group + w, at, :] for w in range(group)]
                    acc = [None] * group
                    for n in range(nstate):
                        into = spread[n, block(b * span + t, CHUNKS), :]
                        outof = spread[nstate + n, block(b * span + t, CHUNKS), :]
                        for w in range(group):
                            i = w * nstate + n
                            factor = decay[b * span + t, g * group + w, pl.ds(n * CHUNKS, CHUNKS), :]
                            held[i] = factor * held[i] + push[w] * into
                            term = held[i] * outof
                            acc[w] = term if acc[w] is None else acc[w] + term
                    for w in range(group):
                        result[g * group + w, at, :] = acc[w]
                    return tuple(held)

                lax.fori_loop(
                    0, span, one,
                    tuple(
                        state[b, g * group + w, pl.ds(n * CHUNKS, CHUNKS), :]
                        for w in range(group) for n in range(nstate)
                    ),
                )

    local_scan(2 if lanes % 2 == 0 else 1)

    @pl.loop(0, lanes)
    def _(k):
        cols = pl.ds(pl.multiple_of(k * LANE, LANE), LANE)
        rate = rate_ref[:, cols]
        for b in range(batch):
            carry = jnp.zeros((nstate, LANE), jnp.float32)
            for c in range(CHUNKS):
                part = state[b, k, pl.ds(c, nstate, stride=CHUNKS), :]
                carry = jnp.exp(-sums[b, k, pl.ds(c, 1), :] * rate) * carry + part
            agg[pl.ds(b * nstate, nstate), cols] = carry.astype(jnp.bfloat16)
            tot[pl.ds(b, 1), cols] = jnp.sum(sums[b, k], axis=0, keepdims=True)

    def pair(source, target):
        device = {"dp": target}
        return (
            remote(agg, agg_in.at[source], s1.at[target], r1.at[source], device),
            remote(tot, tot_in.at[source], s2.at[target], r2.at[source], device),
        )

    for other in range(nd):
        @pl.when(other > me)
        def _():
            for copy in pair(me, other):
                copy.start()

    z_passes()
    for other in range(nd):
        @pl.when(other < me)
        def _():
            for copy in pair(other, me):
                copy.wait_recv()

    @pl.loop(0, lanes)
    def _(k):
        cols = pl.ds(pl.multiple_of(k * LANE, LANE), LANE)
        rate = rate_ref[:, cols]
        for b in range(batch):
            def earlier(d, carry):
                decay = jnp.exp(-tot_in[d, pl.ds(b, 1), cols] * rate)
                return decay * carry + agg_in[d, pl.ds(b * nstate, nstate), cols].astype(
                    jnp.float32
                )

            carry = lax.fori_loop(0, me, earlier, jnp.zeros((nstate, LANE), jnp.float32))
            for c in range(CHUNKS):
                at = pl.ds(c, nstate, stride=CHUNKS)
                part = state[b, k, at, :]
                state[b, k, at, :] = carry
                carry = jnp.exp(-sums[b, k, pl.ds(c, 1), :] * rate) * carry + part

    final_scan(2 if lanes % 2 == 0 else 1)

    @pl.when(core == 0)
    def _():
        remote(tail_of(0), tail_at(core), edge_s.at[0], edge_r.at[core], across).wait_send()

    @pl.when(chip < nd // 2 - 1)
    def _():
        remote(tail_of(1), tail_at(core), edge_s.at[1], edge_r.at[core], onward).wait_send()

    z_waits()
    project(full_z, 1 - core)
    zswap(zswap_s, zswap_r).start()
    project(full_z, core)
    zwhole[:, :, columns(core)] = made[core]
    zswapped(zswap_s, zswap_r).wait_recv()

    @pl.loop(0, lanes)
    def _(k):
        cols = block(k, LANE)
        for b in range(batch):
            gate = zwhole[b, :, cols].astype(jnp.float32)
            at = pl.ds(b * length, length)
            gated_ref[at, cols] = (result[k, at] * (gate / (1.0 + jnp.exp(-gate)))).astype(jnp.bfloat16)

    for other in range(nd):
        @pl.when(other > me)
        def _():
            for copy in pair(me, other):
                copy.wait_send()
    norm_copy.wait_send()
    zswap(zswap_s, zswap_r).wait_send()
    x_sends()
    z_sends()


def front(resid, gain, in_x, in_z, conv_w, conv_b, xdt, xbc, dt_gain, proj, bias, rate, batch, nv, nd):
    rows, width = resid.shape
    chans = in_x.shape[1]
    half = chans // 2
    ranks = proj.shape[0]
    nstate = rate.shape[0]
    lanes = chans // LANE
    length = rows // batch
    cols = ranks + 2 * nstate + -(ranks + 2 * nstate) % LANE
    dma = pltpu.SemaphoreType.DMA
    big = pltpu.VMEM((lanes, rows, LANE), jnp.float32)
    slots = 5 if nd == 8 else nd // 2
    gathers = [dma, dma((slots, 2)), dma((slots, 2)), dma((2, 2)), dma((2, 2))]
    anywhere = pl.BlockSpec(memory_space=pl.ANY)
    return pl.pallas_call(
        functools.partial(front_kernel, nv, nd, batch, ranks, nstate),
        out_shape=jax.ShapeDtypeStruct((rows, chans), jnp.bfloat16),
        in_specs=[VMEM, VMEM, anywhere, anywhere] + [VMEM] * 8,
        out_specs=VMEM,
        scratch_shapes=[
            pltpu.VMEM((2, rows, width), jnp.bfloat16),
            pltpu.VMEM((width, half), jnp.bfloat16),
            pltpu.VMEM((width, half), jnp.bfloat16),
            pltpu.VMEM((2, batch, length, half), jnp.bfloat16),
            pltpu.VMEM((batch, length, chans), jnp.bfloat16),
            pltpu.VMEM((batch, length, chans), jnp.bfloat16),
            pltpu.VMEM((batch, 16, chans), jnp.bfloat16),
            pltpu.VMEM((length + 8, min(256, chans)), jnp.float32),
            pltpu.VMEM((rows, chans), jnp.float32),
            pltpu.VMEM((rows, cols), jnp.bfloat16),
            pltpu.VMEM((nv - 1, rows // nv, cols), jnp.bfloat16),
            pltpu.VMEM((rows // nv, cols), jnp.bfloat16),
            pltpu.VMEM((rows, cols), jnp.bfloat16),
            big, big,
            pltpu.VMEM((rows, cols - ranks), jnp.float32),
            big,
            pltpu.VMEM((rows // CHUNKS, lanes, nstate * CHUNKS, LANE), jnp.float32),
            pltpu.VMEM((2 * nstate, rows, LANE), jnp.float32),
            pltpu.VMEM((batch, lanes, nstate * CHUNKS, LANE), jnp.float32),
            pltpu.VMEM((batch, lanes, CHUNKS, LANE), jnp.float32),
            pltpu.VMEM((batch * nstate, chans), jnp.bfloat16),
            pltpu.VMEM((batch, chans), jnp.float32),
            pltpu.VMEM((nd, batch * nstate, chans), jnp.bfloat16),
            pltpu.VMEM((nd, batch, chans), jnp.float32),
            dma, dma,
        ] + gathers + gathers + [dma, dma, dma((2,)), dma((2,)), dma, dma]
        + [dma((nv - 1,))] * 4 + [dma((nd,))] * 4,
        compiler_params=pltpu.CompilerParams(
            collective_id=2, has_side_effects=True, vmem_limit_bytes=56 * 1024 * 1024
        ),
        cost_estimate=pl.CostEstimate(flops=0, bytes_accessed=int(90 * 3.0e6), transcendentals=0),
        name="front",
    )(resid, gain, in_x, in_z, conv_w, conv_b, xdt, xbc, dt_gain, proj, bias, rate)


def back_kernel(
    nv, nd, steps, relay_at, gated_ref, w_ref, resid_ref, gain_ref, head_ref, ids_ref, lengths_ref,
    hidden_ref, logp_ref, sum_ref,
    weight, own, near, send_up, recv_up, send_down, recv_down, hid, fin, full, logits, ids, stats, heard,
    part, parts, w_sem, near_sem, up_s, up_r, down_s, down_r, gup_s, gup_r, gdown_s, gdown_r,
    fin_s, fin_r, ids_s, ids_r, head_l, head_s, head_r, pass_s, pass_r, stat_s, stat_r, sum_s, sum_r,
):
    me = lax.axis_index("vocab")
    dev = lax.axis_index("dp")
    chip, core = dev // 2, lax.rem(dev, 2)
    mate = {"dp": chip * 2 + 1 - core}
    above, below = {"vocab": lax.rem(me + 1, nv)}, {"vocab": lax.rem(me + nv - 1, nv)}
    rows, chans = gated_ref.shape
    batch, length = ids_ref.shape
    width = w_ref.shape[1]
    share = width // nv
    entries, feats = head_ref.shape
    half = entries // 2
    size = rows // steps

    def block(index, length):
        return pl.ds(pl.multiple_of(index * length, length), length)

    weight_copies = []
    for s in range(nv):
        index = jnp.where(me * 2 < nv, nv - 1 - s, s)
        copy = pltpu.make_async_copy(
            w_ref.at[:, block(index, share)], weight.at[:, block(index, share)], w_sem.at[s]
        )
        copy.start()
        weight_copies.append((index, copy))
    near_copy = pltpu.make_async_copy(resid_ref.at[:, block(me, share)], near, near_sem)
    near_copy.start()
    greet_back(nv, nd)

    head_waits, head_sends, passes = gather_halves(
        nd, lambda c: head_ref.at[block(c, half)], lambda d: full.at[:, block(d, feats)], half,
        head_l, head_s, head_r, pass_s, pass_r,
    )
    mine = ids.at[core]
    ids[core] = ids_ref[...]
    ids_copy = remote(ids_ref, mine, ids_s, ids_r, mate)
    ids_copy.start()

    def up(i, j):
        return remote(send_up.at[i, j - 1], recv_up.at[i, j - 1], up_s.at[i, j - 1], up_r.at[i, j - 1], above)

    def down(i, j):
        return remote(send_down.at[i, j], recv_down.at[i, j], down_s.at[i, j], down_r.at[i, j], below)

    def spread_up(i, s):
        at = hid.at[block(i, size), block(s, share)]
        return remote(at, at, gup_s.at[i, s], gup_r.at[i, s], above)

    def spread_down(i, s):
        at = hid.at[block(i, size), block(s, share)]
        return remote(at, at, gdown_s.at[i, s - 1], gdown_r.at[i, s - 1], below)

    def fin_copy(i):
        at = fin.at[core, block(i, size)]
        return remote(at, at, fin_s.at[i], fin_r.at[i], mate)

    tile = min(512, share)
    for index, copy in weight_copies:
        copy.wait()

        @pl.loop(0, share // tile)
        def _(k):
            at = pl.ds(pl.multiple_of(index * share + k * tile, tile), tile)
            own[:, at] = jnp.dot(gated_ref[...], weight[:, at], preferred_element_type=jnp.float32)

        @pl.when((me == 0) & (index > 0))
        def _():
            @pl.loop(0, steps)
            def _(i):
                send_up[i, index - 1] = own[block(i, size), block(index, share)].astype(jnp.bfloat16)
                up(i, index).start()

        @pl.when((me == nv - 1) & (index < nv - 1))
        def _():
            @pl.loop(0, steps)
            def _(i):
                send_down[i, index] = own[block(i, size), block(index, share)].astype(jnp.bfloat16)
                down(i, index).start()

    near_copy.wait()

    def combine_up(i):
        for j in range(nv - 1, 0, -1):
            @pl.when((me > 0) & (me < j))
            def _():
                up(i, j).wait_recv()
                send_up[i, j - 1] = (
                    own[block(i, size), pl.ds(j * share, share)] + recv_up[i, j - 1].astype(jnp.float32)
                ).astype(jnp.bfloat16)
                up(i, j).start()

    def combine_down(i):
        for j in range(nv - 1):
            @pl.when((me < nv - 1) & (me > j))
            def _():
                down(i, j).wait_recv()
                send_down[i, j] = (
                    own[block(i, size), pl.ds(j * share, share)] + recv_down[i, j].astype(jnp.float32)
                ).astype(jnp.bfloat16)
                down(i, j).start()

    def finish(i):
        at = block(i, size)
        own[at, block(me, share)] = own[at, block(me, share)] + near[at, :].astype(jnp.float32)

        @pl.when(me > 0)
        def _():
            up(i, me).wait_recv()
            own[at, block(me, share)] = own[at, block(me, share)] + recv_up[i, me - 1].astype(jnp.float32)

        @pl.when(me < nv - 1)
        def _():
            down(i, me).wait_recv()
            own[at, block(me, share)] = own[at, block(me, share)] + recv_down[i, me].astype(jnp.float32)

        value = own[at, block(me, share)].astype(jnp.bfloat16)
        hidden_ref[at, :] = value
        hid[at, block(me, share)] = value

        @pl.when(me < nv - 1)
        def _():
            spread_up(i, me).start()

        @pl.when(me > 0)
        def _():
            spread_down(i, me).start()

    def forward(i, hops):
        low, high = me - hops, me + hops

        @pl.when(low >= 0)
        def _():
            spread_up(i, low).wait_recv()

            @pl.when(me < nv - 1)
            def _():
                spread_up(i, low).start()

        @pl.when(high < nv)
        def _():
            spread_down(i, high).wait_recv()

            @pl.when(me > 0)
            def _():
                spread_down(i, high).start()

    def normalize(i):
        at = block(i, size)
        wide = hid[at, :].astype(jnp.float32)
        scale = lax.rsqrt(jnp.mean(wide * wide, axis=-1, keepdims=True) + 1e-05)
        fin[core, at] = (wide * scale * gain_ref[...]).astype(jnp.bfloat16)
        fin_copy(i).start()

    late = jnp.where(me * 2 >= nv, 1, 0)

    def walk(first, last):
        @pl.loop(first, last)
        def _(t):
            def at(i, step):
                @pl.when((i >= 0) & (i < steps))
                def _():
                    step(i)

            at(t - late, combine_up)
            at(t - 1 + late, combine_down)
            at(t - 2, finish)
            for hops in range(1, nv):
                at(t - 2 - hops, functools.partial(forward, hops=hops))
            at(t - 1 - nv, normalize)

    walk(0, relay_at)
    passes()
    walk(relay_at, steps + nv + 1)

    @pl.loop(0, steps)
    def _(i):
        remote(
            fin.at[core, block(i, size)], fin.at[1 - core, block(i, size)], fin_s.at[i], fin_r.at[i], mate
        ).wait_recv()
    ids_copy.wait()
    head_waits()

    vt = min(256, half)
    for s in range(2):
        @pl.loop(0, half // vt)
        def _(k):
            logits[block(k, vt), s * rows : (s + 1) * rows] = lax.dot_general(
                full[block(k, vt), :], fin[s], (((1,), (1,)), ((), ())), preferred_element_type=jnp.float32
            )

        def highest(k, top):
            return jnp.maximum(
                top, jnp.max(logits[block(k, vt), s * rows : (s + 1) * rows], axis=0, keepdims=True)
            )

        top = lax.fori_loop(0, half // vt, highest, jnp.full((1, rows), -jnp.inf, jnp.float32))
        wanted = jnp.concatenate([ids[s, b : b + 1, :] for b in range(batch)], axis=1) - (me * entries + core * half)

        def gather(k, carry):
            total, picked = carry
            values = logits[block(k, vt), s * rows : (s + 1) * rows]
            entry = lax.broadcasted_iota(jnp.int32, values.shape, 0) + k * vt
            total = total + jnp.sum(jnp.exp(values - top), axis=0, keepdims=True)
            picked = picked + jnp.sum(jnp.where(entry == wanted, values, 0.0), axis=0, keepdims=True)
            return total, picked

        zero = jnp.zeros((1, rows), jnp.float32)
        total, picked = lax.fori_loop(0, half // vt, gather, (zero, zero))
        stats[s, 0:1, :] = top
        stats[s, 1:2, :] = total
        stats[s, 2:3, :] = picked
        stats[s, 3:8, :] = jnp.zeros((5, rows), jnp.float32)

    sends = []
    for shift in range(nv):
        for other in range(2):
            if shift == 0 and other == 0:
                continue
            owner = core if other == 0 else 1 - core
            copy = remote(
                stats.at[owner], heard.at[me, core], stat_s.at[shift, other], stat_r.at[me, core],
                {"vocab": lax.rem(me + shift, nv), "dp": chip * 2 + owner},
            )
            copy.start()
            sends.append(copy)
    heard[me, core] = stats[core]
    for z in range(nv):
        for c in range(2):
            @pl.when((z != me) | (c != core))
            def _():
                remote(stats.at[0], heard.at[z, c], stat_s.at[0, 1], stat_r.at[z, c], mate).wait_recv()
    everyone = [heard[z, c] for z in range(nv) for c in range(2)]
    top = everyone[0][0:1]
    for one in everyone[1:]:
        top = jnp.maximum(top, one[0:1])
    total = jnp.zeros_like(top)
    picked = jnp.zeros_like(top)
    for one in everyone:
        total = total + one[1:2] * jnp.exp(one[0:1] - top)
        picked = picked + one[2:3]
    logp = picked - (top + jnp.log(total))
    place = lax.broadcasted_iota(jnp.int32, (1, length), 1) + dev * length
    masked = jnp.zeros((1, 1), jnp.float32)
    count = jnp.zeros((1, 1), jnp.float32)
    for b in range(batch):
        part_logp = logp[:, b * length : (b + 1) * length]
        logp_ref[b : b + 1, :] = part_logp
        masked = masked + jnp.sum(jnp.where(place < lengths_ref[b], part_logp, 0.0), axis=-1, keepdims=True)
        count = count + lengths_ref[b].astype(jnp.float32)
    part[...] = jnp.broadcast_to(masked, part.shape)
    for shift in range(1, nd):
        copy = remote(
            part, parts.at[dev], sum_s.at[shift - 1], sum_r.at[dev], {"dp": lax.rem(dev + shift, nd)}
        )
        copy.start()
        sends.append(copy)
    parts[dev] = part[...]
    for d in range(nd):
        @pl.when(d != dev)
        def _():
            remote(part, parts.at[d], sum_s.at[0], sum_r.at[d], mate).wait_recv()
    grand = parts[0]
    for d in range(1, nd):
        grand = grand + parts[d]
    sum_ref[...] = grand[0:1, 0:1] / count

    for copy in sends:
        copy.wait_send()
    head_sends()

    @pl.loop(0, steps)
    def _(i):
        fin_copy(i).wait_send()
        for j in range(1, nv):
            @pl.when(me < j)
            def _():
                up(i, j).wait_send()
        for j in range(nv - 1):
            @pl.when(me > j)
            def _():
                down(i, j).wait_send()
        for s in range(nv - 1):
            @pl.when((me >= s) & (me < nv - 1))
            def _():
                spread_up(i, s).wait_send()
        for s in range(1, nv):
            @pl.when((me <= s) & (me > 0))
            def _():
                spread_down(i, s).wait_send()


def greet_back(nv, nd):
    barrier = pltpu.get_barrier_semaphore()
    me, dev = lax.axis_index("vocab"), lax.axis_index("dp")
    mate = dev // 2 * 2 + 1 - lax.rem(dev, 2)
    for shift in range(1, nd):
        pl.semaphore_signal(barrier, inc=1, device_id=peer("dp", shift), device_id_type=MESH)
    for shift in range(1, nv):
        z = lax.rem(me + shift, nv)
        pl.semaphore_signal(barrier, inc=1, device_id={"vocab": z}, device_id_type=MESH)
        pl.semaphore_signal(barrier, inc=1, device_id={"vocab": z, "dp": mate}, device_id_type=MESH)
    pl.semaphore_wait(barrier, nd - 1 + 2 * (nv - 1))


def gather_halves(nd, source, target, length, local, send, recv, pass_s, pass_r):
    dev = lax.axis_index("dp")
    chip, core = dev // 2, lax.rem(dev, 2)
    keep = pltpu.make_async_copy(source(core), target(dev), local)
    keep.start()
    copies = [remote(source(1 - core), target(dev), send.at[0, 0], recv.at[0, core], {"dp": chip * 2 + 1 - core})]
    copies[0].start()
    waits = [remote(source(0), target(chip * 2 + 1 - core), send.at[0, 0], recv.at[0, 1 - core], {"dp": dev})]
    if nd != 8:
        for shift in range(1, nd // 2):
            there = lax.rem(chip + shift, nd // 2)
            back = lax.rem(chip + nd // 2 - shift, nd // 2)
            for c in range(2):
                copy = remote(
                    source(c), target(dev), send.at[shift, c], recv.at[shift, core], {"dp": there * 2 + c}
                )
                copy.start()
                copies.append(copy)
                waits.append(
                    remote(source(c), target(back * 2 + c), send.at[shift, c], recv.at[shift, c], {"dp": dev})
                )
        passes = lambda: None
    else:
        piece = length // 2
        sides = (chip + 1 - 2 * lax.rem(chip, 2), lax.rem(chip + 2, 4))

        def at(ref, p):
            return ref.at[pl.ds(p * piece, piece)]

        first = []
        for turn in range(2):
            for side in range(2):
                p = side if turn == 0 else 1 - side
                for c in range(2):
                    k = 1 + side * 2 + p
                    copy = remote(
                        at(source(c), p), at(target(dev), p), send.at[k, c], recv.at[k, core],
                        {"dp": sides[side] * 2 + c},
                    )
                    copy.start()
                    copies.append(copy)
                    came = at(target(sides[side] * 2 + c), p)
                    wait = remote(came, came, send.at[k, c], recv.at[k, c], {"dp": dev})
                    if turn == 0:
                        first.append((side, p, c, wait, came))
                    else:
                        waits.append(wait)

        far = 3 - chip
        for side in range(2):
            for c in range(2):
                came = at(target(far * 2 + c), 1 - side)
                waits.append(
                    remote(came, came, pass_s.at[side, c], pass_r.at[1 - side, c], {"dp": dev})
                )

        def passes():
            for side, p, c, wait, came in first:
                wait.wait_recv()
                copy = remote(
                    came, came, pass_s.at[side, c], pass_r.at[p, c], {"dp": sides[1 - side] * 2 + core}
                )
                copy.start()
                copies.append(copy)

    def finish_waits():
        keep.wait()
        for wait in waits:
            wait.wait_recv()

    def finish_sends():
        for copy in copies:
            copy.wait_send()

    return finish_waits, finish_sends, passes


def back(gated, w, resid, gain, head, ids, lengths, nv, nd, steps=4, relay_at=3):
    rows, chans = gated.shape
    width = w.shape[1]
    share = width // nv
    half = head.shape[0] // 2
    size = rows // steps
    dma = pltpu.SemaphoreType.DMA
    line = pltpu.VMEM((steps, nv - 1, size, share), jnp.bfloat16)
    lanes = 5 if nd == 8 else nd // 2
    anywhere = pl.BlockSpec(memory_space=pl.ANY)
    return pl.pallas_call(
        functools.partial(back_kernel, nv, nd, steps, relay_at),
        out_shape=(
            jax.ShapeDtypeStruct((rows, share), jnp.bfloat16),
            jax.ShapeDtypeStruct(ids.shape, jnp.float32),
            jax.ShapeDtypeStruct((1, 1), jnp.float32),
        ),
        in_specs=[VMEM, anywhere, anywhere, VMEM, anywhere, VMEM, pl.BlockSpec(memory_space=pltpu.SMEM)],
        out_specs=(VMEM, VMEM, VMEM),
        scratch_shapes=[
            pltpu.VMEM((chans, width), jnp.bfloat16),
            pltpu.VMEM((rows, width), jnp.float32),
            pltpu.VMEM((rows, share), jnp.bfloat16),
            line, line, line, line,
            pltpu.VMEM((rows, width), jnp.bfloat16),
            pltpu.VMEM((2, rows, width), jnp.bfloat16),
            pltpu.VMEM((half, width), jnp.bfloat16),
            pltpu.VMEM((half, 2 * rows), jnp.float32),
            pltpu.VMEM((2,) + ids.shape, jnp.int32),
            pltpu.VMEM((2, 8, rows), jnp.float32),
            pltpu.VMEM((nv, 2, 8, rows), jnp.float32),
            pltpu.VMEM((8, LANE), jnp.float32),
            pltpu.VMEM((nd, 8, LANE), jnp.float32),
            dma((nv,)), dma,
        ] + [dma((steps, nv - 1))] * 8 + [
            dma((steps,)), dma((steps,)), dma, dma, dma, dma((lanes, 2)), dma((lanes, 2)),
            dma((2, 2)), dma((2, 2)), dma((nv, 2)), dma((nv, 2)), dma((nd,)), dma((nd,)),
        ],
        compiler_params=pltpu.CompilerParams(
            collective_id=3, has_side_effects=True, vmem_limit_bytes=60 * 1024 * 1024
        ),
        cost_estimate=pl.CostEstimate(flops=0, bytes_accessed=int(80 * 3.0e6), transcendentals=0),
        name="back",
    )(gated, w, resid, gain, head, ids, lengths)


def body(
    resid, norm_gain, in_x, in_z, conv_w, conv_b, xdt_w, xbc_w, dt_gain, dt_proj, dt_bias,
    a_rate, out_w, final_gain, head_w, targets, lengths,
):
    nv, nd = lax.axis_size("vocab"), lax.axis_size("dp")
    batch, local_len, width = resid.shape
    channels = in_x.shape[1]
    rows = batch * local_len

    flat = resid.reshape(rows, width)
    gated = front(
        flat, norm_gain[None, :], in_x, in_z, conv_w, conv_b[None, :], xdt_w, xbc_w.T, dt_gain[None, :], dt_proj,
        dt_bias[None, :], a_rate.T, batch, nv, nd,
    )
    share = width // nv
    hidden_share, logp, mean_logp = back(
        gated, out_w, flat, final_gain[None, :], head_w, targets, lengths, nv, nd
    )
    return (
        hidden_share.reshape(batch, local_len, share),
        logp,
        mean_logp.reshape(()),
    )


def solution(mesh):
    in_specs = (
        P(None, "dp", None), P(), P("dp", "vocab"), P("dp", "vocab"), P(None, "vocab"), P("vocab"),
        P("vocab", None), P("vocab", None), P(), P(None, "vocab"), P("vocab"), P("vocab", None),
        P("vocab", None), P(), P("vocab", "dp"), P(None, "dp"), P(),
    )
    out_specs = (P(None, "dp", "vocab"), P(None, "dp"), P())
    return jax.shard_map(body, mesh=mesh, in_specs=in_specs, out_specs=out_specs, check_vma=False)
```
